128 devices in a mesh: gx: 8 (over x, z_lo), gy: 16 (over z_hi, y, core).
Axes of the slice: x: 4, y: 4, z: 4 (z_hi: 2, z_lo: 2; z = z_hi * 2 + z_lo), core: 2. Of those that a mesh axis runs over, the one named last changes fastest.
Arguments:
- velocity: float32 [2, 4096, 8192], P(None, 'gx', 'gy'), may hold values from -3 to 3
- stress: float32 [3, 4096, 8192], P(None, 'gx', 'gy'), may hold values from -3 to 3
- strength: float32 [4096, 8192], P('gx', 'gy'), may hold values from 0.5 to 4
- ice_mass: float32 [4096, 8192], P('gx', 'gy'), may hold values from 0.3 to 20, as said below
- wind_stress: float32 [2, 4096, 8192], P(None, 'gx', 'gy'), may hold values from -6 to 6
- current: float32 [2, 4096, 8192], P(None, 'gx', 'gy'), may hold values from -3 to 3
- ice_mask: int32 [4096, 8192], P('gx', 'gy'), may hold values from 0 to 1, as said below
- open_water: int32 [4096, 8192], P('gx', 'gy'), may hold values 0 or 1
Outputs:
- new_velocity: float32 [2, 4096, 8192], P(None, 'gx', 'gy')
- new_stress: float32 [3, 4096, 8192], P(None, 'gx', 'gy')
- residual: float32 [], replicated
- kinetic_energy: float32 [], replicated
The draws below stay inside these ranges and needn't reach their ends.
Inputs may be any that keep to these rules, and one draw needn't show every extreme that they name: `ice_mask`: 1 marks an ocean cell, 0 a land cell. `ice_mass`: positive everywhere.
All inputs are finite; a program needn't handle non-finite values. No bound on the sum of `open_water` on one device may be relied on, other than what follows from the above.
Results may differ from the reference program's by a relative error of at most 0.00002.
Values sent between devices are 32-bit elements; how exact they have to be, the bound alone decides.
A program may use at most 128 MiB of HBM per device.

```python
import math
import jax
import jax.numpy as jnp

ITERS = 4
NX = 4096
NY = 8192


def draw_ice_mass(key, part):
    row_ramp = 1.0 + 2.0 * jnp.arange(NX, dtype=jnp.float32) / NX
    col_ramp = 1.0 + 2.0 * jnp.arange(NY, dtype=jnp.float32) / NY
    ramp = row_ramp[:, None] * col_ramp[None, :]
    rough = jax.random.uniform(key, (NX, NY), jnp.float32, 0.6, 1.4)
    return (ramp * rough).astype(jnp.float32)


def draw_ice_mask(key, part):
    row_index = jnp.arange(NX, dtype=jnp.int32)[:, None]
    col_index = jnp.arange(NY, dtype=jnp.int32)[None, :]
    land_cells = jnp.zeros((NX, NY), jnp.int32)
    for number in range(8):
        key_a, key_b, key_c, key_d = jax.random.split(jax.random.fold_in(key, number + 11), 4)
        start_x = jax.random.randint(key_a, (), 0, NX)
        width_x = jax.random.randint(key_b, (), 1, max(NX // 4, 2))
        start_y = jax.random.randint(key_c, (), 0, NY)
        width_y = jax.random.randint(key_d, (), 1, max(NY // 4, 2))
        inside = (row_index >= start_x) & (row_index < start_x + width_x) & (col_index >= start_y) & (col_index < start_y + width_y)
        land_cells = jnp.maximum(land_cells, inside.astype(jnp.int32))
    speckle = (jax.random.randint(jax.random.fold_in(key, 97), (NX, NY), 0, 16) == 0).astype(jnp.int32)
    land_cells = jnp.maximum(land_cells, speckle)
    return (1 - land_cells).astype(jnp.int32)


def set_ends(entries, own_key, low, high):
    longest = entries.shape.index(max(entries.shape))
    spots = []
    for shift in (0, 1):
        where = [jax.random.randint(jax.random.fold_in(own_key, axis), (), 0, length) for axis, length in enumerate(entries.shape)]
        where[longest] = (where[longest] + shift) % entries.shape[longest]
        spots.append(tuple(where))
    return entries.at[spots[0]].set(low).at[spots[1]].set(high)


def levels(key, extent, shards, smallest, high):
    level, own = 1.0, jax.random.fold_in(key, 6)
    for dim, blocks in shards:
        heights = jnp.exp(jax.random.uniform(jax.random.fold_in(own, dim), (blocks,), jnp.float32, smallest / len(shards), high / len(shards)))
        level = level * jnp.repeat(heights, extent[dim] // blocks).reshape([-1 if axis == dim else 1 for axis in range(len(extent))])
    return level


def normal_values(rng, dims, deviation, most, cuts=(), kind=jnp.bfloat16):
    level = levels(rng, dims, cuts, -0.22, 0.18) if cuts else 1.0
    drawn = jax.random.normal(rng, dims, jnp.float32) * deviation * level
    return jnp.minimum(jnp.maximum(drawn, -most), most).astype(kind)


def setup_inputs(seed: int = 0) -> dict:
    key_of = jax.random.split(jax.random.key(seed), 9)
    velocity = normal_values(key_of[0], (2, NX, NY), 0.5, 3.0, ((1, 8), (2, 16)), jnp.float32)
    stress = normal_values(key_of[1], (3, NX, NY), 0.5, 3.0, ((1, 8), (2, 16)), jnp.float32)
    strength = jnp.clip(jnp.exp(math.log(4.0) - 2.0794415 * jax.random.uniform(key_of[2], (NX, NY), jnp.float32) ** levels(key_of[2], (NX, NY), ((0, 8), (1, 16)), -0.2, 0.2)), 0.5, 4.0)
    ice_mass = draw_ice_mass(jax.random.fold_in(key_of[8], 71), 0)
    wind_stress = normal_values(key_of[4], (2, NX, NY), 1.0, 6.0, ((1, 8), (2, 16)), jnp.float32)
    current = normal_values(key_of[5], (2, NX, NY), 0.5, 3.0, ((1, 8), (2, 16)), jnp.float32)
    ice_mask = draw_ice_mask(jax.random.fold_in(key_of[8], 71), 0)
    open_water = set_ends((jax.random.randint(key_of[7], (NX, NY), 0, 8) < 1).astype(jnp.int32), jax.random.fold_in(key_of[7], 1), 0, 1)
    return {"velocity": velocity, "stress": stress, "strength": strength, "ice_mass": ice_mass, "wind_stress": wind_stress, "current": current, "ice_mask": ice_mask, "open_water": open_water}


relax_rate = 0.8
ecc_square = 4.0
delta_floor = 0.05
time_step = 0.5
drag_coef = 1.0
coriolis = 0.3

def corner_diffs(values):
    along_x = (values[1:, 1:] + values[1:, :-1] - values[:-1, 1:] - values[:-1, :-1]) * 0.5
    along_y = (values[1:, 1:] + values[:-1, 1:] - values[1:, :-1] - values[:-1, :-1]) * 0.5
    return (along_x, along_y)

def update_stress(velocity, stress, pressure):
    du_dx, du_dy = corner_diffs(velocity[0])
    dv_dx, dv_dy = corner_diffs(velocity[1])
    divu = du_dx + dv_dy
    tension = du_dx - dv_dy
    shear = du_dy + dv_dx
    deform = jnp.sqrt(divu * divu + (tension * tension + shear * shear) / ecc_square + delta_floor * delta_floor)
    viscous = pressure / deform
    first = (stress[0] + relax_rate * viscous * (divu - deform)) / (1.0 + relax_rate)
    second = (stress[1] + relax_rate * viscous * tension / ecc_square) / (1.0 + relax_rate)
    third = (stress[2] + relax_rate * viscous * shear * 0.5 / ecc_square) / (1.0 + relax_rate)
    return jnp.stack([first, second, third])

def stress_force(stress):
    normal_x = 0.5 * (stress[0] + stress[1])
    normal_y = 0.5 * (stress[0] - stress[1])
    normal_x_dx, unused_x = corner_diffs(normal_x)
    unused_y, normal_y_dy = corner_diffs(normal_y)
    shear_dx, shear_dy = corner_diffs(stress[2])
    return (normal_x_dx + shear_dy, shear_dx + normal_y_dy)

def advance(velocity, force_x, force_y, ice_mass, wind_stress, current, ice_weight):
    inertia = ice_mass / time_step
    diagonal = inertia + drag_coef
    turning = ice_mass * coriolis
    rhs_u = inertia * velocity[0] + force_x + wind_stress[0] + drag_coef * current[0]
    rhs_v = inertia * velocity[1] + force_y + wind_stress[1] + drag_coef * current[1]
    determinant = diagonal * diagonal + turning * turning
    new_u = (diagonal * rhs_u + turning * rhs_v) / determinant * ice_weight
    new_v = (diagonal * rhs_v - turning * rhs_u) / determinant * ice_weight
    return jnp.stack([new_u, new_v])

def reference(velocity, stress, strength, ice_mass, wind_stress, current, ice_mask, open_water):
    ice_weight = ice_mask.astype(jnp.float32) * (1.0 - open_water.astype(jnp.float32))
    pressure = strength * ice_weight
    previous = velocity
    for subcycle in range(ITERS):
        padded = jnp.pad(velocity, ((0, 0), (1, 0), (1, 0)))
        stress = update_stress(padded, stress, pressure)
        force_x, force_y = stress_force(jnp.pad(stress, ((0, 0), (0, 1), (0, 1))))
        previous = velocity
        velocity = advance(velocity, force_x, force_y, ice_mass, wind_stress, current, ice_weight)
    change = velocity - previous
    residual = jnp.sum(ice_weight * (change[0] * change[0] + change[1] * change[1])) / (NX * NY)
    kinetic = 0.5 * jnp.sum(ice_mass * ice_weight * (velocity[0] * velocity[0] + velocity[1] * velocity[1])) / (NX * NY)
    return (velocity, stress, residual, kinetic)
```

```python
import functools

import jax
import jax.numpy as jnp
from jax import lax
from jax.experimental import pallas as pl
from jax.experimental.pallas import tpu as pltpu
from jax.sharding import Mesh
from jax.sharding import PartitionSpec as P

ITERS = 4
GX = ("gx_0", "gx_1")
GY = ("gy_0", "gy_1", "gy_2")
AXES = GX + GY

relax_rate = 0.8
ecc_square = 4.0
delta_floor = 0.05
time_step = 0.5
drag_coef = 1.0
coriolis = 0.3

F32 = jnp.float32
LANES = 128
CHUNKS = 8
FIELDS = 11
U, V, A, B, T, PR, AL, BE, IN, KU, KV = range(FIELDS)
SWAPPED = (V, U, B, A, T, PR, AL, BE, IN, KV, KU)
STRIP_ROWS = 56
TOP_HALO, TOP_OWN, BOT_OWN, BOT_HALO = 8, 16, 32, 40

DECAY = 1.0 / (1.0 + relax_rate)
FLOOR = 4.0 * delta_floor * delta_floor


def lane_ids():
    return lax.broadcasted_iota(jnp.int32, (8, LANES), 1)


def row_ids():
    return lax.broadcasted_iota(jnp.int32, (8, LANES), 0)


def from_left(blocks):
    first = lane_ids() == 0
    rolled = [pltpu.roll(x, 1, 1) for x in blocks]
    return [jnp.where(first, rolled[b - 1], rolled[b]) for b in range(len(blocks))]


def from_right(blocks):
    last = lane_ids() == LANES - 1
    rolled = [pltpu.roll(x, LANES - 1, 1) for x in blocks]
    count = len(blocks)
    return [jnp.where(last, rolled[(b + 1) % count], rolled[b]) for b in range(count)]


class Domain:
    def __init__(self, blocks, get):
        self.blocks = blocks
        self.get = get

    def read(self, field, level, row):
        ref = self.get(field, level)
        return [ref[b, pl.ds(row, 8), :] for b in range(self.blocks)]

    def write(self, field, level, row, values):
        ref = self.get(field, level)
        for b in range(self.blocks):
            ref[b, pl.ds(row, 8), :] = values[b]


def stress_phase(dom, level, row):
    n = dom.blocks
    u, um = dom.read(U, level, row), dom.read(U, level, row - 1)
    v, vm = dom.read(V, level, row), dom.read(V, level, row - 1)
    pr = dom.read(PR, 0, row)
    sa, sb, st = (dom.read(f, level, row) for f in (A, B, T))
    m1, m2, m3, m4 = [], [], [], []
    for b in range(n):
        du, su = u[b] - um[b], u[b] + um[b]
        dv, sv = v[b] - vm[b], v[b] + vm[b]
        m1.append(du + sv)
        m2.append(du - sv)
        m3.append(su + dv)
        m4.append(su - dv)
    l1, l2, l4 = from_left(m1), from_left(m2), from_left(m4)
    na, nb, nt = [], [], []
    for b in range(n):
        div = m1[b] + l2[b]
        ten = m2[b] + l1[b]
        she = m3[b] - l4[b]
        ten4, she4 = 0.25 * ten, 0.25 * she
        rate = lax.rsqrt((div * div + FLOOR) + (ten * ten4 + she * she4))
        vis = pr[b] * rate
        e1 = vis * div - pr[b]
        e2 = vis * ten4
        na.append(DECAY * sa[b] + (e1 + e2))
        nb.append(DECAY * sb[b] + (e1 - e2))
        nt.append(DECAY * st[b] + vis * she4)
    dom.write(A, level + 1, row, na)
    dom.write(B, level + 1, row, nb)
    dom.write(T, level + 1, row, nt)
    return na, nb, nt


def velocity_phase(dom, level, row):
    n = dom.blocks
    sa, sap = dom.read(A, level + 1, row), dom.read(A, level + 1, row + 1)
    sb, sbp = dom.read(B, level + 1, row), dom.read(B, level + 1, row + 1)
    st, stp = dom.read(T, level + 1, row), dom.read(T, level + 1, row + 1)
    e, g, h, j = [], [], [], []
    for b in range(n):
        da, sumt = sap[b] - sa[b], stp[b] + st[b]
        dt, sumb = stp[b] - st[b], sbp[b] + sb[b]
        e.append(da + sumt)
        g.append(da - sumt)
        h.append(dt + sumb)
        j.append(dt - sumb)
    re, rh = from_right(e), from_right(h)
    u, v = dom.read(U, level, row), dom.read(V, level, row)
    al, be, inert = (dom.read(f, 0, row) for f in (AL, BE, IN))
    ku, kv = dom.read(KU, 0, row), dom.read(KV, 0, row)
    nu, nv = [], []
    for b in range(n):
        ru = inert[b] * u[b] + (re[b] + g[b]) + ku[b]
        rv = inert[b] * v[b] + (rh[b] + j[b]) + kv[b]
        nu.append(al[b] * ru + be[b] * rv)
        nv.append(al[b] * rv - be[b] * ru)
    dom.write(U, level + 1, row, nu)
    dom.write(V, level + 1, row, nv)
    return u, v, nu, nv, inert


def square_sums(phase, keep):
    res, kin = None, None
    for u, v, nu, nv, inert, mask in zip(*phase, keep):
        if mask is False:
            continue
        du, dv = nu - u, nv - v
        r = du * du + dv * dv
        k = inert * (nu * nu + nv * nv)
        if mask is not None:
            r, k = jnp.where(mask, r, 0.0), jnp.where(mask, k, 0.0)
        res = r if res is None else res + r
        kin = k if kin is None else kin + k
    return res, kin


def wavefront(tiles, phases, carry, arrive=None):
    depth = max(lag for lag, _ in phases)

    def step(t, carry, active):
        if arrive is not None and active[0][0] == 0:
            arrive(t)
        for lag, phase in reversed(active):
            carry = phase(t - lag, carry)
        return carry

    for t in range(depth):
        carry = step(t, carry, [p for p in phases if p[0] <= t])
    carry = lax.fori_loop(depth, tiles, lambda t, c: step(t, c, phases), carry)
    for t in range(tiles, tiles + depth):
        carry = step(t, carry, [p for p in phases if t - p[0] < tiles])
    return carry


def main_kernel(
    vel, stress, strength, mass, wind, current, mask, water,
    out_vel, out_str, out_sum,
    uv0, str_in, strength_in, mass_in, wind_in, cur_in, mask_in, water_in,
    uv1, uv2, uv3, uv4, s0, s1, s2, s3, s4, coef,
    packed, rows0, rows_uv, rows_s, cols0, cols_uv, cols_s, turned,
    in_sem, send_sem, recv_sem,
):
    nrow, ncol = mass.shape
    nblk = ncol // LANES
    tiles = nrow // 8
    per = nrow // CHUNKS
    row_blks = nrow // LANES
    gx, gy = lax.axis_index(GX), lax.axis_index(GY)
    ngx, ngy = lax.axis_size(GX), lax.axis_size(GY)

    def copies(c):
        r = pl.ds(c * per, per)
        out = []
        for b in range(nblk):
            out.append((vel.at[:, r, b * LANES : (b + 1) * LANES], uv0.at[:, b, pl.ds(c * per + 8, per), :]))
        for src, dst in ((stress, str_in), (wind, wind_in), (current, cur_in)):
            out.append((src.at[:, r, :], dst.at[:, r, :]))
        for src, dst in ((strength, strength_in), (mass, mass_in), (mask, mask_in), (water, water_in)):
            out.append((src.at[r, :], dst.at[r, :]))
        return [pltpu.make_async_copy(s, d, in_sem.at[i, c]) for i, (s, d) in enumerate(out)]

    for c in [0, CHUNKS - 1] + list(range(1, CHUNKS - 1)):
        for copy in copies(c):
            copy.start()

    def peer(axis, step):
        if axis == 0:
            x, y = lax.rem(gx + step + ngx, ngx), gy
        else:
            x, y = gx, lax.rem(gy + step + ngy, ngy)
        ids = {}
        for names, index in ((GX, x), (GY, y)):
            for name in reversed(names):
                size = lax.axis_size(name)
                ids[name] = lax.rem(index, size)
                index = lax.div(index, size)
        return tuple(ids[name] for name in AXES)

    barrier = pltpu.get_barrier_semaphore()
    for axis in (0, 1):
        for step in (-1, 1):
            pl.semaphore_signal(barrier, 1, device_id=peer(axis, step), device_id_type=pl.DeviceIdType.MESH)

    def prologue(row, b):
        r, l = pl.ds(row, 8), slice(b * LANES, (b + 1) * LANES)
        ice = mask_in[r, l] > water_in[r, l]
        m = mass_in[r, l]
        diag, turn = m * (1.0 / time_step) + drag_coef, m * coriolis
        inv = jnp.where(ice, 0.25 / (diag * diag + turn * turn), 0.0)
        first, second = str_in[0, r, l], str_in[1, r, l]
        pres = jnp.where(ice, strength_in[r, l] * (relax_rate * DECAY), 0.0)
        at = pl.ds(row + 8, 8)
        return [
            uv0[0, b, at, :], uv0[1, b, at, :],
            first + second, first - second, 2.0 * str_in[2, r, l],
            pres, diag * inv, turn * inv, m * (4.0 / time_step),
            4.0 * (wind_in[0, r, l] + drag_coef * cur_in[0, r, l]),
            4.0 * (wind_in[1, r, l] + drag_coef * cur_in[1, r, l]),
        ]

    for c in (0, CHUNKS - 1):
        for copy in copies(c):
            copy.wait()
    for row, at in ((0, TOP_OWN), (nrow - 8, BOT_OWN)):
        for b in range(nblk):
            for f, x in enumerate(prologue(row, b)):
                rows0[f, b, pl.ds(at, 8), :] = x

    def exchange(strip, axis):
        out = []
        for way, (step, src, dst) in enumerate(((-1, TOP_OWN, BOT_HALO), (1, BOT_OWN + 4, TOP_HALO + 4))):
            out.append(
                pltpu.make_async_remote_copy(
                    src_ref=strip.at[:, :, pl.ds(src, 4), :],
                    dst_ref=strip.at[:, :, pl.ds(dst, 4), :],
                    send_sem=send_sem.at[axis, way],
                    recv_sem=recv_sem.at[axis, way],
                    device_id=peer(axis, step),
                    device_id_type=pl.DeviceIdType.MESH,
                )
            )
        return out

    def no_outside(strip, index, count):
        @pl.when(index == 0)
        def _():
            strip[:, :, TOP_HALO : TOP_HALO + 8, :] = jnp.zeros_like(strip[:, :, TOP_HALO : TOP_HALO + 8, :])

        @pl.when(index == count - 1)
        def _():
            strip[:, :, BOT_HALO : BOT_HALO + 8, :] = jnp.zeros_like(strip[:, :, BOT_HALO : BOT_HALO + 8, :])

    pl.semaphore_wait(barrier, 4)
    row_copies = exchange(rows0, 0)
    for copy in row_copies:
        copy.start()

    uvs, ss = (uv0, uv1, uv2, uv3, uv4), (s0, s1, s2, s3, s4)

    def main_get(field, level):
        if field in (U, V):
            return uvs[level].at[field]
        if field in (A, B, T):
            return ss[level].at[field - A]
        return coef.at[field - PR]

    main = Domain(nblk, main_get)
    lane = lane_ids()

    def pack(tile_fields, shift):
        out = None
        for slot, f in enumerate(SWAPPED):
            x = tile_fields[f]
            by = (8 * slot + shift) % LANES
            x = pltpu.roll(x, by, 1) if by else x
            out = x if out is None else jnp.where(lane < 8 * slot, out, x)
        return out

    def arrive(tile):
        if isinstance(tile, int):
            c = tile * 8 // per
            if tile * 8 % per == 0 and c not in (0, CHUNKS - 1):
                for copy in copies(c):
                    copy.wait()
        else:
            c = lax.div(tile, per // 8)

            @pl.when((lax.rem(tile, per // 8) == 0) & (c > 0) & (c < CHUNKS - 1))
            def _():
                for copy in copies(c):
                    copy.wait()

    def prepare(tile, carry):
        row = tile * 8 if isinstance(tile, int) else pl.multiple_of(tile * 8, 8)
        at = row + 8
        for b in range(nblk):
            fields = prologue(row, b)
            for f in (A, B, T):
                s0[f - A, b, pl.ds(at, 8), :] = fields[f]
            for f in range(PR, FIELDS):
                coef[f - PR, b, pl.ds(at, 8), :] = fields[f]
            if b == 0:
                packed[0, pl.ds(row, 8), :] = pack(fields, 0)
            if b == nblk - 1:
                packed[1, pl.ds(row, 8), :] = pack(fields, 8)
        return carry

    def at_row(tile):
        return tile * 8 + 8 if isinstance(tile, int) else pl.multiple_of(tile * 8 + 8, 8)

    def stress_at(level):
        def phase(tile, carry):
            stress_phase(main, level, at_row(tile))
            return carry

        return phase

    def velocity_at(level):
        def phase(tile, carry):
            velocity_phase(main, level, at_row(tile))
            return carry

        return phase

    def put_stress(tile, blocks):
        na, nb, nt = blocks
        r = pl.ds(tile * 8, 8) if isinstance(tile, int) else pl.ds(pl.multiple_of(tile * 8, 8), 8)
        for b in range(nblk):
            l = slice(b * LANES, (b + 1) * LANES)
            out_str[0, r, l] = 0.5 * (na[b] + nb[b])
            out_str[1, r, l] = 0.5 * (na[b] - nb[b])
            out_str[2, r, l] = 0.5 * nt[b]

    def last_stress(tile, carry):
        put_stress(tile, stress_phase(main, ITERS - 1, at_row(tile)))
        return carry

    inner = [None] * nblk
    inner[0] = lane >= 4
    inner[nblk - 1] = lane < LANES - 4

    def last_velocity(tile, carry):
        u, v, nu, nv, inert = velocity_phase(main, ITERS - 1, at_row(tile))
        r = pl.ds(tile * 8, 8) if isinstance(tile, int) else pl.ds(pl.multiple_of(tile * 8, 8), 8)
        for b in range(nblk):
            l = slice(b * LANES, (b + 1) * LANES)
            out_vel[0, r, l] = nu[b]
            out_vel[1, r, l] = nv[b]
        res, kin = square_sums((u, v, nu, nv, inert), inner)
        keep = jnp.int32(0) + row_ids() + tile * 8
        good = (keep >= 4) & (keep < nrow - 4)
        return carry[0] + jnp.where(good, res, 0.0), carry[1] + jnp.where(good, kin, 0.0)

    zero = jnp.zeros((8, LANES), F32)
    wavefront(
        tiles,
        [(0, prepare), (1, stress_at(0)), (3, velocity_at(0)), (4, stress_at(1)), (6, velocity_at(1))],
        0,
        arrive,
    )

    for copy in row_copies:
        copy.wait()
    no_outside(rows0, gx, ngx)
    for side, b, shift in ((0, 0, 0), (1, nblk - 1, 8)):
        for at, to in ((BOT_HALO, nrow), (TOP_HALO, nrow + LANES - 8)):
            packed[side, pl.ds(to, 8), :] = pack([rows0[f, b, pl.ds(at, 8), :] for f in range(FIELDS)], shift)
        for blk in range(row_blks + 1):
            flat = packed[side, pl.ds(blk * LANES, LANES), :].T
            for f in range(FIELDS):
                x = flat[8 * f : 8 * f + 8, :]
                cols0[f, blk, pl.ds((TOP_OWN, BOT_OWN)[side], 8), :] = -x if f == BE else x
    col_copies = exchange(cols0, 1)
    for copy in col_copies:
        copy.start()

    sums = wavefront(
        tiles,
        [(0, stress_at(2)), (2, velocity_at(2)), (3, last_stress), (5, last_velocity)],
        (zero, zero),
    )

    def strip_get(first, uv, s):
        def get(field, level):
            if level == 0:
                return first.at[field]
            return uv.at[level - 1, field] if field in (U, V) else s.at[level - 1, field - A]

        return get

    def sweep_strip(dom):
        own = {}
        for level in range(ITERS):
            for at in (TOP_HALO, TOP_OWN, BOT_OWN, BOT_HALO):
                stress_phase(dom, level, at)
            for at in (TOP_HALO, TOP_OWN, BOT_OWN, BOT_HALO):
                own[at] = velocity_phase(dom, level, at)
        return own

    def add(sums, more):
        return sums[0] + more[0], sums[1] + more[1]

    sub = row_ids()
    row_dom = Domain(nblk, strip_get(rows0, rows_uv, rows_s))
    own = sweep_strip(row_dom)
    for at, row, good in ((TOP_OWN, 0, sub < 4), (BOT_OWN, nrow - 8, sub >= 4)):
        keep = [good if m is None else good & m for m in inner]
        sums = add(sums, square_sums(own[at], keep))
        _, _, nu, nv, _ = own[at]
        sa, sb, st = (row_dom.read(f, ITERS, at) for f in (A, B, T))
        for b in range(nblk):
            r, l = pl.ds(row, 8), slice(b * LANES, (b + 1) * LANES)
            for ref, i, x in (
                (out_vel, 0, nu[b]), (out_vel, 1, nv[b]),
                (out_str, 0, 0.5 * (sa[b] + sb[b])), (out_str, 1, 0.5 * (sa[b] - sb[b])), (out_str, 2, 0.5 * st[b]),
            ):
                ref[i, r, l] = jnp.where(good, x, ref[i, r, l])

    for copy in col_copies:
        copy.wait()
    no_outside(cols0, gy, ngy)
    col_dom = Domain(row_blks + 1, strip_get(cols0, cols_uv, cols_s))
    own = sweep_strip(col_dom)
    for side, (at, good) in enumerate(((TOP_OWN, sub < 4), (BOT_OWN, sub >= 4))):
        sums = add(sums, square_sums(own[at], [good] * row_blks + [False]))
        _, _, nu, nv, _ = own[at]
        sa, sb, st = (col_dom.read(f, ITERS, at) for f in (A, B, T))
        for blk in range(row_blks):
            values = (
                nv[blk], nu[blk],
                0.5 * (sb[blk] + sa[blk]), 0.5 * (sb[blk] - sa[blk]), 0.5 * st[blk],
            )
            for i, x in enumerate(values):
                turned[blk, pl.ds(40 * side + 8 * i, 8), :] = x
    for blk in range(row_blks):
        packed[0, pl.ds(blk * LANES, LANES), :] = turned[blk].T

    def merge(tile, carry):
        r = pl.ds(pl.multiple_of(tile * 8, 8), 8)
        x = packed[0, r, :]
        places = [((out_vel, i) if i < 2 else (out_str, i - 2)) for i in range(5)]
        first, last = slice(0, LANES), slice(ncol - LANES, ncol)
        new = []
        for i, (ref, at) in enumerate(places):
            left = pltpu.roll(x, (LANES - 8 * i) % LANES, 1) if i else x
            right = pltpu.roll(x, (LANES - 8 - 40 - 8 * i) % LANES, 1)
            if first == last:
                new.append((ref, at, first, jnp.where(lane < 4, left, jnp.where(lane >= LANES - 4, right, ref[at, r, first]))))
            else:
                new.append((ref, at, first, jnp.where(lane < 4, left, ref[at, r, first])))
                new.append((ref, at, last, jnp.where(lane >= LANES - 4, right, ref[at, r, last])))
        for ref, at, l, value in new:
            ref[at, r, l] = value
        return carry

    lax.fori_loop(0, tiles, merge, 0, unroll=4)
    out_sum[0] = sums[0]
    out_sum[1] = sums[1]


def per_device(velocity, stress, strength, ice_mass, wind_stress, current, ice_mask, open_water):
    nrow, ncol = ice_mass.shape
    nblk = ncol // LANES
    row_blks = nrow // LANES
    pad = nrow + 16
    vmem = pltpu.VMEM
    any_spec = pl.BlockSpec(memory_space=pl.ANY)
    vmem_spec = pl.BlockSpec(memory_space=pltpu.VMEM)
    new_velocity, new_stress, parts = pl.pallas_call(
        main_kernel,
        out_shape=(
            jax.ShapeDtypeStruct(velocity.shape, F32),
            jax.ShapeDtypeStruct(stress.shape, F32),
            jax.ShapeDtypeStruct((2, 8, LANES), F32),
        ),
        in_specs=[any_spec] * 8,
        out_specs=(vmem_spec, vmem_spec, vmem_spec),
        scratch_shapes=[
            vmem((2, nblk, pad, LANES), F32),
            vmem((3, nrow, ncol), F32),
            vmem((nrow, ncol), F32),
            vmem((nrow, ncol), F32),
            vmem((2, nrow, ncol), F32),
            vmem((2, nrow, ncol), F32),
            vmem((nrow, ncol), jnp.int32),
            vmem((nrow, ncol), jnp.int32),
        ]
        + [vmem((2, nblk, pad, LANES), F32)] * ITERS
        + [vmem((3, nblk, pad, LANES), F32)] * (ITERS + 1)
        + [
            vmem((FIELDS - PR, nblk, pad, LANES), F32),
            vmem((2, nrow + LANES, LANES), F32),
            vmem((FIELDS, nblk, STRIP_ROWS, LANES), F32),
            vmem((ITERS, 2, nblk, STRIP_ROWS, LANES), F32),
            vmem((ITERS, 3, nblk, STRIP_ROWS, LANES), F32),
            vmem((FIELDS, row_blks + 1, STRIP_ROWS, LANES), F32),
            vmem((ITERS, 2, row_blks + 1, STRIP_ROWS, LANES), F32),
            vmem((ITERS, 3, row_blks + 1, STRIP_ROWS, LANES), F32),
            vmem((row_blks, LANES, LANES), F32),
            pltpu.SemaphoreType.DMA((nblk + 7, CHUNKS)),
            pltpu.SemaphoreType.DMA((2, 2)),
            pltpu.SemaphoreType.DMA((2, 2)),
        ],
        compiler_params=pltpu.CompilerParams(
            collective_id=0, has_side_effects=True, vmem_limit_bytes=62 * 1024 * 1024
        ),
        name="subcycles",
    )(velocity, stress, strength, ice_mass, wind_stress, current, ice_mask, open_water)
    totals = lax.psum(jnp.sum(parts, axis=(1, 2)), AXES)
    cells = nrow * lax.axis_size(GX) * ncol * lax.axis_size(GY)
    return (
        new_velocity,
        new_stress,
        totals[0] / cells,
        totals[1] * (0.5 * time_step / 4.0) / cells,
    )


def solution(mesh):
    split = Mesh(mesh.devices.reshape(4, 2, 2, 4, 2), AXES)
    return jax.shard_map(
        per_device,
        mesh=split,
        in_specs=(
            P(None, GX, GY),
            P(None, GX, GY),
            P(GX, GY),
            P(GX, GY),
            P(None, GX, GY),
            P(None, GX, GY),
            P(GX, GY),
            P(GX, GY),
        ),
        out_specs=(P(None, GX, GY), P(None, GX, GY), P(), P()),
        check_vma=False,
    )
```

```python
import functools

import jax
import jax.numpy as jnp
from jax import lax
from jax.experimental import pallas as pl
from jax.experimental.pallas import tpu as pltpu
from jax.sharding import Mesh
from jax.sharding import PartitionSpec as P

ITERS = 4
GX = ("gx_0", "gx_1")
GY = ("gy_0", "gy_1", "gy_2")
AXES = GX + GY

relax_rate = 0.8
ecc_square = 4.0
delta_floor = 0.05
time_step = 0.5
drag_coef = 1.0
coriolis = 0.3

F32 = jnp.float32
LANES = 128
CHUNKS = 8
AHEAD = 3
TALL = 16
FIELDS = 11
U, V, A, B, T, PR, AL, BE, IN, KU, KV = range(FIELDS)
SWAPPED = (V, U, B, A, T, PR, AL, BE, IN, KV, KU)
STRIP_ROWS = 40
TOP_HALO, TOP_OWN, BOT_OWN, BOT_HALO = 8, 12, 20, 28

DECAY = 1.0 / (1.0 + relax_rate)
FLOOR = 4.0 * delta_floor * delta_floor


def lane_ids(height=8):
    return lax.broadcasted_iota(jnp.int32, (height, LANES), 1)


def row_ids(height=8):
    return lax.broadcasted_iota(jnp.int32, (height, LANES), 0)


def from_left(blocks):
    first = lane_ids(blocks[0].shape[0]) == 0
    rolled = [pltpu.roll(x, 1, 1) for x in blocks]
    return [jnp.where(first, rolled[b - 1], rolled[b]) for b in range(len(blocks))]


def from_right(blocks):
    last = lane_ids(blocks[0].shape[0]) == LANES - 1
    rolled = [pltpu.roll(x, LANES - 1, 1) for x in blocks]
    count = len(blocks)
    return [jnp.where(last, rolled[(b + 1) % count], rolled[b]) for b in range(count)]


class Domain:
    def __init__(self, blocks, get, height=8):
        self.blocks = blocks
        self.height = height
        self.get = get

    def read(self, field, level, row):
        ref = self.get(field, level)
        return [ref[b, pl.ds(row, self.height), :] for b in range(self.blocks)]

    def write(self, field, level, row, values):
        ref = self.get(field, level)
        for b in range(self.blocks):
            ref[b, pl.ds(row, self.height), :] = values[b]


def stress_phase(dom, level, row):
    n = dom.blocks
    u, um = dom.read(U, level, row), dom.read(U, level, row - 1)
    v, vm = dom.read(V, level, row), dom.read(V, level, row - 1)
    pr = dom.read(PR, 0, row)
    sa, sb, st = (dom.read(f, level, row) for f in (A, B, T))
    m1, m2, m3, m4 = [], [], [], []
    for b in range(n):
        du, su = u[b] - um[b], u[b] + um[b]
        dv, sv = v[b] - vm[b], v[b] + vm[b]
        m1.append(du + sv)
        m2.append(du - sv)
        m3.append(su + dv)
        m4.append(su - dv)
    l1, l2, l4 = from_left(m1), from_left(m2), from_left(m4)
    na, nb, nt = [], [], []
    for b in range(n):
        div = m1[b] + l2[b]
        ten = m2[b] + l1[b]
        she = m3[b] - l4[b]
        ten4, she4 = 0.25 * ten, 0.25 * she
        rate = lax.rsqrt((div * div + FLOOR) + (ten * ten4 + she * she4))
        vis = pr[b] * rate
        e1 = vis * div - pr[b]
        e2 = vis * ten4
        na.append(DECAY * sa[b] + (e1 + e2))
        nb.append(DECAY * sb[b] + (e1 - e2))
        nt.append(DECAY * st[b] + vis * she4)
    dom.write(A, level + 1, row, na)
    dom.write(B, level + 1, row, nb)
    dom.write(T, level + 1, row, nt)
    return na, nb, nt


def velocity_phase(dom, level, row):
    n = dom.blocks
    sa, sap = dom.read(A, level + 1, row), dom.read(A, level + 1, row + 1)
    sb, sbp = dom.read(B, level + 1, row), dom.read(B, level + 1, row + 1)
    st, stp = dom.read(T, level + 1, row), dom.read(T, level + 1, row + 1)
    e, g, h, j = [], [], [], []
    for b in range(n):
        da, sumt = sap[b] - sa[b], stp[b] + st[b]
        dt, sumb = stp[b] - st[b], sbp[b] + sb[b]
        e.append(da + sumt)
        g.append(da - sumt)
        h.append(dt + sumb)
        j.append(dt - sumb)
    re, rh = from_right(e), from_right(h)
    u, v = dom.read(U, level, row), dom.read(V, level, row)
    al, be, inert = (dom.read(f, 0, row) for f in (AL, BE, IN))
    ku, kv = dom.read(KU, 0, row), dom.read(KV, 0, row)
    nu, nv = [], []
    for b in range(n):
        ru = inert[b] * u[b] + (re[b] + g[b]) + ku[b]
        rv = inert[b] * v[b] + (rh[b] + j[b]) + kv[b]
        nu.append(al[b] * ru + be[b] * rv)
        nv.append(al[b] * rv - be[b] * ru)
    dom.write(U, level + 1, row, nu)
    dom.write(V, level + 1, row, nv)
    return u, v, nu, nv, inert


def square_sums(phase, keep):
    res, kin = None, None
    for u, v, nu, nv, inert, mask in zip(*phase, keep):
        if mask is False:
            continue
        du, dv = nu - u, nv - v
        r = du * du + dv * dv
        k = inert * (nu * nu + nv * nv)
        if mask is not None:
            r, k = jnp.where(mask, r, 0.0), jnp.where(mask, k, 0.0)
        res = r if res is None else res + r
        kin = k if kin is None else kin + k
    return res, kin


def wavefront(tiles, phases, carry, arrive=None):
    depth = max(lag for lag, _ in phases)

    def step(t, carry, active):
        if arrive is not None and active[0][0] == 0:
            arrive(t)
        for lag, phase in reversed(active):
            carry = phase(t - lag, carry)
        return carry

    for t in range(depth):
        carry = step(t, carry, [p for p in phases if p[0] <= t])
    carry = lax.fori_loop(depth, tiles, lambda t, c: step(t, c, phases), carry)
    for t in range(tiles, tiles + depth):
        carry = step(t, carry, [p for p in phases if t - p[0] < tiles])
    return carry


def main_kernel(
    vel, stress, strength, mass, wind, current, mask, water,
    out_vel, out_str, out_res, out_kin,
    uv0, str_in, strength_in, mass_in, wind_in, cur_in, mask_in, water_in,
    uv1, uv2, uv3, uv4, s0, s1, s2, s3, s4, coef,
    packed, rows0, rows_uv, rows_s, cols0, cols_uv, cols_s, turned,
    gather_x, gather_y, in_sem, send_sem, recv_sem, sum_send, sum_recv,
):
    nrow, ncol = mass.shape
    nblk = ncol // LANES
    tiles = nrow // TALL
    per = nrow // CHUNKS
    row_blks = nrow // LANES
    gx, gy = lax.axis_index(GX), lax.axis_index(GY)
    ngx, ngy = lax.axis_size(GX), lax.axis_size(GY)

    def copies(c):
        r = pl.ds(c * per, per)
        out = []
        for b in range(nblk):
            out.append((vel.at[:, r, b * LANES : (b + 1) * LANES], uv0.at[:, b, pl.ds(c * per + 8, per), :]))
        for src, dst in ((stress, str_in), (wind, wind_in), (current, cur_in)):
            out.append((src.at[:, r, :], dst.at[:, r, :]))
        for src, dst in ((strength, strength_in), (mass, mass_in), (mask, mask_in), (water, water_in)):
            out.append((src.at[r, :], dst.at[r, :]))
        return [pltpu.make_async_copy(s, d, in_sem.at[i, c]) for i, (s, d) in enumerate(out)]

    for c in [0, CHUNKS - 1] + list(range(1, AHEAD)):
        for copy in copies(c):
            copy.start()

    def peer(axis, step):
        if axis == 0:
            x, y = lax.rem(gx + step + ngx, ngx), gy
        else:
            x, y = gx, lax.rem(gy + step + ngy, ngy)
        ids = {}
        for names, index in ((GX, x), (GY, y)):
            for name in reversed(names):
                size = lax.axis_size(name)
                ids[name] = lax.rem(index, size)
                index = lax.div(index, size)
        return tuple(ids[name] for name in AXES)

    barrier = pltpu.get_barrier_semaphore()
    for axis, count in ((0, ngx), (1, ngy)):
        for step in range(1, count):
            pl.semaphore_signal(barrier, 1, device_id=peer(axis, step), device_id_type=pl.DeviceIdType.MESH)

    def prologue(row, b, height):
        r, l = pl.ds(row, height), slice(b * LANES, (b + 1) * LANES)
        ice = mask_in[r, l] > water_in[r, l]
        m = mass_in[r, l]
        diag, turn = m * (1.0 / time_step) + drag_coef, m * coriolis
        inv = jnp.where(ice, 0.25 / (diag * diag + turn * turn), 0.0)
        first, second = str_in[0, r, l], str_in[1, r, l]
        pres = jnp.where(ice, strength_in[r, l] * (relax_rate * DECAY), 0.0)
        at = pl.ds(row + 8, height)
        return [
            uv0[0, b, at, :], uv0[1, b, at, :],
            first + second, first - second, 2.0 * str_in[2, r, l],
            pres, diag * inv, turn * inv, m * (4.0 / time_step),
            4.0 * (wind_in[0, r, l] + drag_coef * cur_in[0, r, l]),
            4.0 * (wind_in[1, r, l] + drag_coef * cur_in[1, r, l]),
        ]

    for c in (0, CHUNKS - 1):
        for copy in copies(c):
            copy.wait()
    for row, at in ((0, TOP_OWN), (nrow - 8, BOT_OWN)):
        for b in range(nblk):
            for f, x in enumerate(prologue(row, b, 8)):
                rows0[f, b, pl.ds(at, 8), :] = x

    def exchange(strip, axis):
        out = []
        for way, (step, src, dst) in enumerate(((-1, TOP_OWN, BOT_HALO), (1, BOT_OWN + 4, TOP_HALO))):
            out.append(
                pltpu.make_async_remote_copy(
                    src_ref=strip.at[:, :, pl.ds(src, 4), :],
                    dst_ref=strip.at[:, :, pl.ds(dst, 4), :],
                    send_sem=send_sem.at[axis, way],
                    recv_sem=recv_sem.at[axis, way],
                    device_id=peer(axis, step),
                    device_id_type=pl.DeviceIdType.MESH,
                )
            )
        return out

    def no_outside(strip, index, count):
        @pl.when(index == 0)
        def _():
            strip[:, :, TOP_HALO : TOP_HALO + 4, :] = jnp.zeros(strip.shape[:2] + (4, LANES), F32)

        @pl.when(index == count - 1)
        def _():
            strip[:, :, BOT_HALO : BOT_HALO + 4, :] = jnp.zeros(strip.shape[:2] + (4, LANES), F32)

    pl.semaphore_wait(barrier, ngx + ngy - 2)
    row_copies = exchange(rows0, 0)
    for copy in row_copies:
        copy.start()

    uvs, ss = (uv0, uv1, uv2, uv3, uv4), (s0, s1, s2, s3, s4)

    def main_get(field, level):
        if field in (U, V):
            return uvs[level].at[field]
        if field in (A, B, T):
            return ss[level].at[field - A]
        return coef.at[field - PR]

    main = Domain(nblk, main_get, TALL)
    lane = lane_ids()
    tall_lane = lane_ids(TALL)

    def pack(tile_fields, shift):
        out = None
        for slot, f in enumerate(SWAPPED):
            x = tile_fields[f]
            by = (8 * slot + shift) % LANES
            x = pltpu.roll(x, by, 1) if by else x
            out = x if out is None else jnp.where(lane_ids(x.shape[0]) < 8 * slot, out, x)
        return out

    def arrive(tile):
        if isinstance(tile, int):
            c = tile * TALL // per
            if tile * TALL % per == 0:
                if 0 < c < CHUNKS - 1:
                    for copy in copies(c):
                        copy.wait()
                if c + AHEAD < CHUNKS - 1:
                    for copy in copies(c + AHEAD):
                        copy.start()
        else:
            c = lax.div(tile, per // TALL)
            first = lax.rem(tile, per // TALL) == 0

            @pl.when(first & (c > 0) & (c < CHUNKS - 1))
            def _():
                for copy in copies(c):
                    copy.wait()

            @pl.when(first & (c < CHUNKS - 1 - AHEAD))
            def _():
                for copy in copies(c + AHEAD):
                    copy.start()

    def prepare(tile, carry):
        row = tile * TALL if isinstance(tile, int) else pl.multiple_of(tile * TALL, 8)
        at = row + 8
        for b in range(nblk):
            fields = prologue(row, b, TALL)
            for f in (A, B, T):
                s0[f - A, b, pl.ds(at, TALL), :] = fields[f]
            for f in range(PR, FIELDS):
                coef[f - PR, b, pl.ds(at, TALL), :] = fields[f]
            if b == 0:
                packed[0, pl.ds(row, TALL), :] = pack(fields, 0)
            if b == nblk - 1:
                packed[1, pl.ds(row, TALL), :] = pack(fields, 8)
        return carry

    def at_row(tile):
        return tile * TALL + 8 if isinstance(tile, int) else pl.multiple_of(tile * TALL + 8, 8)

    def stress_at(level):
        def phase(tile, carry):
            stress_phase(main, level, at_row(tile))
            return carry

        return phase

    def velocity_at(level):
        def phase(tile, carry):
            velocity_phase(main, level, at_row(tile))
            return carry

        return phase

    def put_stress(tile, blocks):
        na, nb, nt = blocks
        r = pl.ds(at_row(tile) - 8, TALL)
        for b in range(nblk):
            l = slice(b * LANES, (b + 1) * LANES)
            out_str[0, r, l] = 0.5 * (na[b] + nb[b])
            out_str[1, r, l] = 0.5 * (na[b] - nb[b])
            out_str[2, r, l] = 0.5 * nt[b]

    def last_stress(tile, carry):
        put_stress(tile, stress_phase(main, ITERS - 1, at_row(tile)))
        return carry

    tall_inner = [None] * nblk
    tall_inner[0] = tall_lane >= 4
    tall_inner[nblk - 1] = tall_lane < LANES - 4

    def last_velocity(tile, carry):
        u, v, nu, nv, inert = velocity_phase(main, ITERS - 1, at_row(tile))
        r = pl.ds(at_row(tile) - 8, TALL)
        for b in range(nblk):
            l = slice(b * LANES, (b + 1) * LANES)
            out_vel[0, r, l] = nu[b]
            out_vel[1, r, l] = nv[b]
        res, kin = square_sums((u, v, nu, nv, inert), tall_inner)
        keep = row_ids(TALL) + tile * TALL
        good = (keep >= 4) & (keep < nrow - 4)
        return carry[0] + jnp.where(good, res, 0.0), carry[1] + jnp.where(good, kin, 0.0)

    zero = jnp.zeros((TALL, LANES), F32)
    wavefront(
        tiles,
        [(0, prepare), (1, stress_at(0)), (3, velocity_at(0)), (4, stress_at(1)), (6, velocity_at(1))],
        0,
        arrive,
    )

    for copy in row_copies:
        copy.wait()
    no_outside(rows0, gx, ngx)
    for side, b, shift in ((0, 0, 0), (1, nblk - 1, 8)):
        for at, to in ((BOT_HALO, nrow), (TOP_HALO - 4, nrow + LANES - 8)):
            packed[side, pl.ds(to, 8), :] = pack([rows0[f, b, pl.ds(at, 8), :] for f in range(FIELDS)], shift)
        for blk in range(row_blks + 1):
            flat = packed[side, pl.ds(blk * LANES, LANES), :].T
            for f in range(FIELDS):
                x = flat[8 * f : 8 * f + 8, :]
                cols0[f, blk, pl.ds((TOP_OWN, BOT_OWN)[side], 8), :] = -x if f == BE else x
    col_copies = exchange(cols0, 1)
    for copy in col_copies:
        copy.start()

    sums = wavefront(
        tiles,
        [(0, stress_at(2)), (2, velocity_at(2)), (3, last_stress), (5, last_velocity)],
        (zero, zero),
    )

    def strip_get(first, uv, s):
        def get(field, level):
            if level == 0:
                return first.at[field]
            return uv.at[level - 1, field] if field in (U, V) else s.at[level - 1, field - A]

        return get

    def sweep_strip(dom):
        ends = {}
        for level in range(ITERS):
            for at in (8, 16, 24):
                stress_phase(dom, level, at)
            for at in (8, 16, 24) if level < ITERS - 1 else (8, 24):
                ends[at] = velocity_phase(dom, level, at)
        return ends

    def add(sums, more):
        return sums[0] + more[0], sums[1] + more[1]

    sub = row_ids()
    sums = [sum(x[8 * i : 8 * i + 8] for i in range(TALL // 8)) for x in sums]
    inner = [None] * nblk
    inner[0] = lane >= 4
    inner[nblk - 1] = lane < LANES - 4
    row_dom = Domain(nblk, strip_get(rows0, rows_uv, rows_s))
    ends = sweep_strip(row_dom)
    for at, good in ((8, sub >= 4), (24, sub < 4)):
        sums = add(sums, square_sums(ends[at], [good if m is None else good & m for m in inner]))
    for at, row, good in ((TOP_OWN, 0, sub < 4), (BOT_OWN, nrow - 8, sub >= 4)):
        nu, nv = (row_dom.read(f, ITERS, at) for f in (U, V))
        sa, sb, st = (row_dom.read(f, ITERS, at) for f in (A, B, T))
        for b in range(nblk):
            r, l = pl.ds(row, 8), slice(b * LANES, (b + 1) * LANES)
            for ref, i, x in (
                (out_vel, 0, nu[b]), (out_vel, 1, nv[b]),
                (out_str, 0, 0.5 * (sa[b] + sb[b])), (out_str, 1, 0.5 * (sa[b] - sb[b])), (out_str, 2, 0.5 * st[b]),
            ):
                ref[i, r, l] = jnp.where(good, x, ref[i, r, l])

    for copy in col_copies:
        copy.wait()
    no_outside(cols0, gy, ngy)
    col_dom = Domain(row_blks + 1, strip_get(cols0, cols_uv, cols_s))
    ends = sweep_strip(col_dom)
    for at, good in ((8, sub >= 4), (24, sub < 4)):
        sums = add(sums, square_sums(ends[at], [good] * row_blks + [False]))

    half = LANES // 2
    both = [x + pltpu.roll(x, half, 1) for x in sums]
    mine = jnp.where(lane < half, both[0], both[1])
    gather_x[gx, 0:1, :] = jnp.sum(mine, axis=0, keepdims=True)

    def spread(axis, slots, me, count):
        return [
            pltpu.make_async_remote_copy(
                src_ref=slots.at[me, pl.ds(0, 1), :],
                dst_ref=slots.at[me, pl.ds(0, 1), :],
                send_sem=sum_send.at[axis, d],
                recv_sem=sum_recv.at[axis, d],
                device_id=peer(axis, d),
                device_id_type=pl.DeviceIdType.MESH,
            )
            for d in range(1, count)
        ]

    for side, at in enumerate((TOP_OWN, BOT_OWN)):
        nu, nv = (col_dom.read(f, ITERS, at) for f in (U, V))
        sa, sb, st = (col_dom.read(f, ITERS, at) for f in (A, B, T))
        for blk in range(row_blks):
            values = (
                nv[blk], nu[blk],
                0.5 * (sb[blk] + sa[blk]), 0.5 * (sb[blk] - sa[blk]), 0.5 * st[blk],
            )
            for i, x in enumerate(values):
                turned[blk, pl.ds(40 * side + 8 * i, 8), :] = x
    x_copies = spread(0, gather_x, gx, ngx)
    for copy in x_copies:
        copy.start()
    for blk in range(row_blks):
        packed[0, pl.ds(blk * LANES, LANES), :] = turned[blk].T

    def merge(tile, carry):
        r = pl.ds(pl.multiple_of(tile * 8, 8), 8)
        x = packed[0, r, :]
        places = [((out_vel, i) if i < 2 else (out_str, i - 2)) for i in range(5)]
        first, last = slice(0, LANES), slice(ncol - LANES, ncol)
        new = []
        for i, (ref, at) in enumerate(places):
            left = pltpu.roll(x, (LANES - 8 * i) % LANES, 1) if i else x
            right = pltpu.roll(x, (LANES - 8 - 40 - 8 * i) % LANES, 1)
            if first == last:
                new.append((ref, at, first, jnp.where(lane < 4, left, jnp.where(lane >= LANES - 4, right, ref[at, r, first]))))
            else:
                new.append((ref, at, first, jnp.where(lane < 4, left, ref[at, r, first])))
                new.append((ref, at, last, jnp.where(lane >= LANES - 4, right, ref[at, r, last])))
        for ref, at, l, value in new:
            ref[at, r, l] = value
        return carry

    lax.fori_loop(0, nrow // 16, merge, 0, unroll=4)
    for copy in x_copies:
        copy.wait()
    gather_y[gy, 0:1, :] = sum(gather_x[i, 0:1, :] for i in range(ngx))
    y_copies = spread(1, gather_y, gy, ngy)
    for copy in y_copies:
        copy.start()
    lax.fori_loop(nrow // 16, nrow // 8, merge, 0, unroll=4)
    for copy in y_copies:
        copy.wait()
    total = sum(gather_y[i, 0:1, :] for i in range(ngy))
    cells = nrow * ngx * ncol * ngy
    low = lax.broadcasted_iota(jnp.int32, (1, LANES), 1) < half
    out_res[0, 0] = jnp.sum(jnp.where(low, total, 0.0)) * (1.0 / cells)
    out_kin[0, 0] = jnp.sum(jnp.where(low, 0.0, total)) * (0.5 * time_step / 4.0 / cells)


def per_device(velocity, stress, strength, ice_mass, wind_stress, current, ice_mask, open_water):
    nrow, ncol = ice_mass.shape
    nblk = ncol // LANES
    row_blks = nrow // LANES
    pad = nrow + 16
    vmem = pltpu.VMEM
    any_spec = pl.BlockSpec(memory_space=pl.ANY)
    vmem_spec = pl.BlockSpec(memory_space=pltpu.VMEM)
    smem_spec = pl.BlockSpec(memory_space=pltpu.SMEM)
    ngx, ngy = lax.axis_size(GX), lax.axis_size(GY)
    new_velocity, new_stress, residual, kinetic = pl.pallas_call(
        main_kernel,
        out_shape=(
            vmem(velocity.shape, F32),
            vmem(stress.shape, F32),
            jax.ShapeDtypeStruct((1, 1), F32),
            jax.ShapeDtypeStruct((1, 1), F32),
        ),
        in_specs=[any_spec] * 8,
        out_specs=(vmem_spec, vmem_spec, smem_spec, smem_spec),
        scratch_shapes=[
            vmem((2, nblk, pad, LANES), F32),
            vmem((3, nrow, ncol), F32),
            vmem((nrow, ncol), F32),
            vmem((nrow, ncol), F32),
            vmem((2, nrow, ncol), F32),
            vmem((2, nrow, ncol), F32),
            vmem((nrow, ncol), jnp.int32),
            vmem((nrow, ncol), jnp.int32),
        ]
        + [vmem((2, nblk, pad, LANES), F32)] * ITERS
        + [vmem((3, nblk, pad, LANES), F32)] * (ITERS + 1)
        + [
            vmem((FIELDS - PR, nblk, pad, LANES), F32),
            vmem((2, nrow + LANES, LANES), F32),
            vmem((FIELDS, nblk, STRIP_ROWS, LANES), F32),
            vmem((ITERS, 2, nblk, STRIP_ROWS, LANES), F32),
            vmem((ITERS, 3, nblk, STRIP_ROWS, LANES), F32),
            vmem((FIELDS, row_blks + 1, STRIP_ROWS, LANES), F32),
            vmem((ITERS, 2, row_blks + 1, STRIP_ROWS, LANES), F32),
            vmem((ITERS, 3, row_blks + 1, STRIP_ROWS, LANES), F32),
            vmem((row_blks, LANES, LANES), F32),
            vmem((ngx, 8, LANES), F32),
            vmem((ngy, 8, LANES), F32),
            pltpu.SemaphoreType.DMA((nblk + 7, CHUNKS)),
            pltpu.SemaphoreType.DMA((2, 2)),
            pltpu.SemaphoreType.DMA((2, 2)),
            pltpu.SemaphoreType.DMA((2, max(ngx, ngy))),
            pltpu.SemaphoreType.DMA((2, max(ngx, ngy))),
        ],
        compiler_params=pltpu.CompilerParams(
            collective_id=0, has_side_effects=True, vmem_limit_bytes=57 * 1024 * 1024
        ),
        name="subcycles",
    )(velocity, stress, strength, ice_mass, wind_stress, current, ice_mask, open_water)
    return new_velocity, new_stress, residual.reshape(()), kinetic.reshape(())


def solution(mesh):
    split = Mesh(mesh.devices.reshape(4, 2, 2, 4, 2), AXES)
    return jax.shard_map(
        per_device,
        mesh=split,
        in_specs=(
            P(None, GX, GY),
            P(None, GX, GY),
            P(GX, GY),
            P(GX, GY),
            P(None, GX, GY),
            P(None, GX, GY),
            P(GX, GY),
            P(GX, GY),
        ),
        out_specs=(P(None, GX, GY), P(None, GX, GY), P(), P()),
        check_vma=False,
    )
```

```python
import functools

import jax
import jax.numpy as jnp
from jax import lax
from jax.experimental import pallas as pl
from jax.experimental.pallas import tpu as pltpu
from jax.sharding import Mesh
from jax.sharding import PartitionSpec as P

ITERS = 4
GX = ("gx_0", "gx_1")
GY = ("gy_0", "gy_1", "gy_2")
AXES = GX + GY

relax_rate = 0.8
ecc_square = 4.0
delta_floor = 0.05
time_step = 0.5
drag_coef = 1.0
coriolis = 0.3

F32 = jnp.float32
LANES = 128
CHUNKS = 8
AHEAD = 3
MIDWAY = 3
TALL = 16
FIELDS = 11
U, V, A, B, T, PR, AL, BE, IN, KU, KV = range(FIELDS)
SWAPPED = (V, U, B, A, T, PR, AL, BE, IN, KV, KU)
SPLIT = 6
STRIP_ROWS = 40
TOP_HALO, TOP_OWN, BOT_OWN, BOT_HALO = 8, 12, 20, 28

DECAY = 1.0 / (1.0 + relax_rate)
FLOOR = 4.0 * delta_floor * delta_floor


def lane_ids(height=8):
    return lax.broadcasted_iota(jnp.int32, (height, LANES), 1)


def row_ids(height=8):
    return lax.broadcasted_iota(jnp.int32, (height, LANES), 0)


def from_left(blocks):
    first = lane_ids(blocks[0].shape[0]) == 0
    rolled = [pltpu.roll(x, 1, 1) for x in blocks]
    return [jnp.where(first, rolled[b - 1], rolled[b]) for b in range(len(blocks))]


def from_right(blocks):
    last = lane_ids(blocks[0].shape[0]) == LANES - 1
    rolled = [pltpu.roll(x, LANES - 1, 1) for x in blocks]
    count = len(blocks)
    return [jnp.where(last, rolled[(b + 1) % count], rolled[b]) for b in range(count)]


class Domain:
    def __init__(self, blocks, get, height=8):
        self.blocks = blocks
        self.height = height
        self.get = get

    def read(self, field, level, row):
        ref = self.get(field, level)
        return [ref[b, pl.ds(row, self.height), :] for b in range(self.blocks)]

    def write(self, field, level, row, values):
        ref = self.get(field, level)
        for b in range(self.blocks):
            ref[b, pl.ds(row, self.height), :] = values[b]


def stress_phase(dom, level, row):
    n = dom.blocks
    u, um = dom.read(U, level, row), dom.read(U, level, row - 1)
    v, vm = dom.read(V, level, row), dom.read(V, level, row - 1)
    pr = dom.read(PR, 0, row)
    sa, sb, st = (dom.read(f, level, row) for f in (A, B, T))
    m1, m2, m3, m4 = [], [], [], []
    for b in range(n):
        du, su = u[b] - um[b], u[b] + um[b]
        dv, sv = v[b] - vm[b], v[b] + vm[b]
        m1.append(du + sv)
        m2.append(du - sv)
        m3.append(su + dv)
        m4.append(su - dv)
    l1, l2, l4 = from_left(m1), from_left(m2), from_left(m4)
    na, nb, nt = [], [], []
    for b in range(n):
        div = m1[b] + l2[b]
        ten = m2[b] + l1[b]
        she = m3[b] - l4[b]
        ten4, she4 = 0.25 * ten, 0.25 * she
        rate = lax.rsqrt((div * div + FLOOR) + (ten * ten4 + she * she4))
        vis = pr[b] * rate
        e1 = vis * div - pr[b]
        e2 = vis * ten4
        na.append(DECAY * sa[b] + (e1 + e2))
        nb.append(DECAY * sb[b] + (e1 - e2))
        nt.append(DECAY * st[b] + vis * she4)
    dom.write(A, level + 1, row, na)
    dom.write(B, level + 1, row, nb)
    dom.write(T, level + 1, row, nt)
    return na, nb, nt


def velocity_phase(dom, level, row):
    n = dom.blocks
    sa, sap = dom.read(A, level + 1, row), dom.read(A, level + 1, row + 1)
    sb, sbp = dom.read(B, level + 1, row), dom.read(B, level + 1, row + 1)
    st, stp = dom.read(T, level + 1, row), dom.read(T, level + 1, row + 1)
    e, g, h, j = [], [], [], []
    for b in range(n):
        da, sumt = sap[b] - sa[b], stp[b] + st[b]
        dt, sumb = stp[b] - st[b], sbp[b] + sb[b]
        e.append(da + sumt)
        g.append(da - sumt)
        h.append(dt + sumb)
        j.append(dt - sumb)
    re, rh = from_right(e), from_right(h)
    u, v = dom.read(U, level, row), dom.read(V, level, row)
    al, be, inert = (dom.read(f, 0, row) for f in (AL, BE, IN))
    ku, kv = dom.read(KU, 0, row), dom.read(KV, 0, row)
    nu, nv = [], []
    for b in range(n):
        ru = inert[b] * u[b] + (re[b] + g[b]) + ku[b]
        rv = inert[b] * v[b] + (rh[b] + j[b]) + kv[b]
        nu.append(al[b] * ru + be[b] * rv)
        nv.append(al[b] * rv - be[b] * ru)
    dom.write(U, level + 1, row, nu)
    dom.write(V, level + 1, row, nv)
    return u, v, nu, nv, inert


def square_sums(phase, keep):
    res, kin = None, None
    for u, v, nu, nv, inert, mask in zip(*phase, keep):
        if mask is False:
            continue
        du, dv = nu - u, nv - v
        r = du * du + dv * dv
        k = inert * (nu * nu + nv * nv)
        if mask is not None:
            r, k = jnp.where(mask, r, 0.0), jnp.where(mask, k, 0.0)
        res = r if res is None else res + r
        kin = k if kin is None else kin + k
    return res, kin


def wavefront(tiles, phases, carry, arrive=None, group=1, midway=None):
    depth = max(lag for lag, _ in phases)

    def step(t, carry, active):
        for lag, phase in active:
            carry = phase(t - lag, carry)
        return carry

    def steady(t, carry):
        return step(t, carry, phases)

    for t in range(depth):
        if arrive is not None and t % group == 0:
            arrive(t // group)
        carry = step(t, carry, [p for p in phases if p[0] <= t])
    if arrive is None:
        carry = lax.fori_loop(depth, tiles, steady, carry)
    else:
        whole = -(-depth // group)
        if depth < whole * group:
            carry = lax.fori_loop(depth, whole * group, steady, carry)

        def run_group(c, carry):
            arrive(c)
            return lax.fori_loop(c * group, (c + 1) * group, steady, carry)

        carry = lax.fori_loop(whole, MIDWAY, run_group, carry)
        midway()
        carry = lax.fori_loop(MIDWAY, tiles // group, run_group, carry)
    for t in range(tiles, tiles + depth):
        carry = step(t, carry, [p for p in phases if t - p[0] < tiles])
    return carry


def main_kernel(
    vel, stress, strength, mass, wind, current, mask, water,
    out_vel, out_str, out_res, out_kin,
    uv0, str_in, strength_in, mass_in, wind_in, cur_in, mask_in, water_in,
    uv1, uv2, uv3, uv4, s0, s1, s2, s3, s4, coef,
    packed, rows0, rows_uv, rows_s, cols0, cols_uv, cols_s, turned,
    gather_x, gather_y, in_sem, send_sem, recv_sem, sum_send, sum_recv,
):
    nrow, ncol = mass.shape
    nblk = ncol // LANES
    tiles = nrow // TALL
    per = nrow // CHUNKS
    row_blks = nrow // LANES
    gx, gy = lax.axis_index(GX), lax.axis_index(GY)
    ngx, ngy = lax.axis_size(GX), lax.axis_size(GY)

    def copies(c):
        r = pl.ds(c * per, per)
        out = []
        for b in range(nblk):
            out.append((vel.at[:, r, b * LANES : (b + 1) * LANES], uv0.at[:, b, pl.ds(c * per + 8, per), :]))
        for src, dst in ((stress, str_in), (wind, wind_in), (current, cur_in)):
            out.append((src.at[:, r, :], dst.at[:, r, :]))
        for src, dst in ((strength, strength_in), (mass, mass_in), (mask, mask_in), (water, water_in)):
            out.append((src.at[r, :], dst.at[r, :]))
        return [pltpu.make_async_copy(s, d, in_sem.at[i, c]) for i, (s, d) in enumerate(out)]

    for c in list(range(AHEAD)) + [CHUNKS - 1]:
        for copy in copies(c):
            copy.start()

    def peer(axis, step):
        if axis == 0:
            x, y = lax.rem(gx + step + ngx, ngx), gy
        else:
            x, y = gx, lax.rem(gy + step + ngy, ngy)
        ids = {}
        for names, index in ((GX, x), (GY, y)):
            for name in reversed(names):
                size = lax.axis_size(name)
                ids[name] = lax.rem(index, size)
                index = lax.div(index, size)
        return tuple(ids[name] for name in AXES)

    barrier = pltpu.get_barrier_semaphore()
    for axis, count in ((0, ngx), (1, ngy)):
        for step in range(1, count):
            pl.semaphore_signal(barrier, 1, device_id=peer(axis, step), device_id_type=pl.DeviceIdType.MESH)

    def prologue(row, b, height):
        r, l = pl.ds(row, height), slice(b * LANES, (b + 1) * LANES)
        ice = mask_in[r, l] > water_in[r, l]
        m = mass_in[r, l]
        diag, turn = m * (1.0 / time_step) + drag_coef, m * coriolis
        inv = jnp.where(ice, 0.25 / (diag * diag + turn * turn), 0.0)
        first, second = str_in[0, r, l], str_in[1, r, l]
        pres = jnp.where(ice, strength_in[r, l] * (relax_rate * DECAY), 0.0)
        at = pl.ds(row + 8, height)
        return [
            uv0[0, b, at, :], uv0[1, b, at, :],
            first + second, first - second, 2.0 * str_in[2, r, l],
            pres, diag * inv, turn * inv, m * (4.0 / time_step),
            4.0 * (wind_in[0, r, l] + drag_coef * cur_in[0, r, l]),
            4.0 * (wind_in[1, r, l] + drag_coef * cur_in[1, r, l]),
        ]

    def exchange(strip, axis):
        out = []
        for way, (step, src, dst) in enumerate(((-1, TOP_OWN, BOT_HALO), (1, BOT_OWN + 4, TOP_HALO))):
            out.append(
                pltpu.make_async_remote_copy(
                    src_ref=strip.at[:, :, pl.ds(src, 4), :],
                    dst_ref=strip.at[:, :, pl.ds(dst, 4), :],
                    send_sem=send_sem.at[axis, way],
                    recv_sem=recv_sem.at[axis, way],
                    device_id=peer(axis, step),
                    device_id_type=pl.DeviceIdType.MESH,
                )
            )
        return out

    def no_outside(strip, index, count):
        @pl.when(index == 0)
        def _():
            strip[:, :, TOP_HALO : TOP_HALO + 4, :] = jnp.zeros(strip.shape[:2] + (4, LANES), F32)

        @pl.when(index == count - 1)
        def _():
            strip[:, :, BOT_HALO : BOT_HALO + 4, :] = jnp.zeros(strip.shape[:2] + (4, LANES), F32)

    row_copies = exchange(rows0, 0)

    def send_rows():
        for copy in copies(CHUNKS - 1):
            copy.wait()
        for row, at in ((0, TOP_OWN), (nrow - 8, BOT_OWN)):
            for b in range(nblk):
                for f, x in enumerate(prologue(row, b, 8)):
                    rows0[f, b, pl.ds(at, 8), :] = x
        pl.semaphore_wait(barrier, ngx + ngy - 2)
        for copy in row_copies:
            copy.start()

    uvs, ss = (uv0, uv1, uv2, uv3, uv4), (s0, s1, s2, s3, s4)

    def main_get(field, level):
        if field in (U, V):
            return uvs[level].at[field]
        if field in (A, B, T):
            return ss[level].at[field - A]
        return coef.at[field - PR]

    main = Domain(nblk, main_get, TALL)
    lane = lane_ids()
    tall_lane = lane_ids(TALL)

    def pack(first, last):
        lanes = lane_ids(first[0].shape[0])
        out = []
        for names in (SWAPPED[:SPLIT], SWAPPED[SPLIT:]):
            edges = [jnp.where(lanes < LANES // 2, first[f], last[f]) for f in names]
            total = pltpu.roll(edges[1], 16, 1)
            for q in range(2, len(edges)):
                total = jnp.where(lanes < 16 * q - 8, total, pltpu.roll(edges[q], 16 * q, 1))
            out.append(jnp.where((lanes < 8) | (lanes >= LANES - 8), edges[0], total))
        return out

    def arrive(c):
        if isinstance(c, int):
            if c < CHUNKS - 1:
                for copy in copies(c):
                    copy.wait()
            if c + AHEAD < CHUNKS - 1:
                for copy in copies(c + AHEAD):
                    copy.start()
        else:

            @pl.when(c < CHUNKS - 1)
            def _():
                for copy in copies(c):
                    copy.wait()

            @pl.when(c < CHUNKS - 1 - AHEAD)
            def _():
                for copy in copies(c + AHEAD):
                    copy.start()

    def prepare(tile, carry):
        row = tile * TALL if isinstance(tile, int) else pl.multiple_of(tile * TALL, 8)
        at = row + 8
        edges = []
        for b in range(nblk):
            fields = prologue(row, b, TALL)
            for f in (A, B, T):
                s0[f - A, b, pl.ds(at, TALL), :] = fields[f]
            for f in range(PR, FIELDS):
                coef[f - PR, b, pl.ds(at, TALL), :] = fields[f]
            if b in (0, nblk - 1):
                edges.append(fields)
        for i, x in enumerate(pack(edges[0], edges[-1])):
            packed[i, pl.ds(row, TALL), :] = x
        return carry

    def at_row(tile):
        return tile * TALL + 8 if isinstance(tile, int) else pl.multiple_of(tile * TALL + 8, 8)

    def stress_at(level):
        def phase(tile, carry):
            stress_phase(main, level, at_row(tile))
            return carry

        return phase

    def velocity_at(level):
        def phase(tile, carry):
            velocity_phase(main, level, at_row(tile))
            return carry

        return phase

    def put_stress(tile, blocks):
        na, nb, nt = blocks
        r = pl.ds(at_row(tile) - 8, TALL)
        for b in range(nblk):
            l = slice(b * LANES, (b + 1) * LANES)
            out_str[0, r, l] = 0.5 * (na[b] + nb[b])
            out_str[1, r, l] = 0.5 * (na[b] - nb[b])
            out_str[2, r, l] = 0.5 * nt[b]

    def last_stress(tile, carry):
        put_stress(tile, stress_phase(main, ITERS - 1, at_row(tile)))
        return carry

    tall_inner = [None] * nblk
    tall_inner[0] = tall_lane >= 4
    tall_inner[nblk - 1] = tall_lane < LANES - 4

    def last_velocity(tile, carry):
        u, v, nu, nv, inert = velocity_phase(main, ITERS - 1, at_row(tile))
        r = pl.ds(at_row(tile) - 8, TALL)
        for b in range(nblk):
            l = slice(b * LANES, (b + 1) * LANES)
            out_vel[0, r, l] = nu[b]
            out_vel[1, r, l] = nv[b]
        res, kin = square_sums((u, v, nu, nv, inert), tall_inner)
        keep = row_ids(TALL) + tile * TALL
        good = (keep >= 4) & (keep < nrow - 4)
        return carry[0] + jnp.where(good, res, 0.0), carry[1] + jnp.where(good, kin, 0.0)

    zero = jnp.zeros((TALL, LANES), F32)
    wavefront(
        tiles,
        [(6, velocity_at(1)), (4, stress_at(1)), (3, velocity_at(0)), (1, stress_at(0)), (0, prepare)],
        0,
        arrive,
        per // TALL,
        send_rows,
    )

    for copy in row_copies:
        copy.wait()
    no_outside(rows0, gx, ngx)
    for at, to in ((BOT_HALO, nrow), (TOP_HALO - 4, nrow + LANES - 8)):
        ends = [[rows0[f, b, pl.ds(at, 8), :] for f in range(FIELDS)] for b in (0, nblk - 1)]
        for i, x in enumerate(pack(*ends)):
            packed[i, pl.ds(to, 8), :] = x
    for i, names in enumerate((range(SPLIT), range(SPLIT, FIELDS))):
        for blk in range(row_blks + 1):
            flat = packed[i, pl.ds(blk * LANES, LANES), :].T
            for q, f in enumerate(names):
                for at, to in ((16 * q, TOP_OWN), ((16 * q - 8) % LANES, BOT_OWN)):
                    x = flat[at : at + 8, :]
                    cols0[f, blk, pl.ds(to, 8), :] = -x if f == BE else x
    col_copies = exchange(cols0, 1)
    for copy in col_copies:
        copy.start()

    sums = wavefront(
        tiles,
        [(5, last_velocity), (3, last_stress), (2, velocity_at(2)), (0, stress_at(2))],
        (zero, zero),
    )

    def strip_get(first, uv, s):
        def get(field, level):
            if level == 0:
                return first.at[field]
            return uv.at[level - 1, field] if field in (U, V) else s.at[level - 1, field - A]

        return get

    for copy in col_copies:
        copy.wait()
    no_outside(cols0, gy, ngy)
    row_dom = Domain(nblk, strip_get(rows0, rows_uv, rows_s))
    col_dom = Domain(row_blks + 1, strip_get(cols0, cols_uv, cols_s))
    row_ends, col_ends = {}, {}
    for level in range(ITERS):
        for at in (8, 16, 24):
            stress_phase(row_dom, level, at)
            stress_phase(col_dom, level, at)
        for at in (8, 16, 24) if level < ITERS - 1 else (8, 24):
            row_ends[at] = velocity_phase(row_dom, level, at)
            col_ends[at] = velocity_phase(col_dom, level, at)

    def add(sums, more):
        return sums[0] + more[0], sums[1] + more[1]

    sub = row_ids()
    sums = [sum(x[8 * i : 8 * i + 8] for i in range(TALL // 8)) for x in sums]
    inner = [None] * nblk
    inner[0] = lane >= 4
    inner[nblk - 1] = lane < LANES - 4
    for at, good in ((8, sub >= 4), (24, sub < 4)):
        sums = add(sums, square_sums(row_ends[at], [good if m is None else good & m for m in inner]))
        sums = add(sums, square_sums(col_ends[at], [good] * row_blks + [False]))

    half = LANES // 2
    both = [x + pltpu.roll(x, half, 1) for x in sums]
    mine = jnp.where(lane < half, both[0], both[1])
    gather_x[gx, 0:1, :] = jnp.sum(mine, axis=0, keepdims=True)

    def spread(axis, slots, me, count):
        return [
            pltpu.make_async_remote_copy(
                src_ref=slots.at[me, pl.ds(0, 1), :],
                dst_ref=slots.at[me, pl.ds(0, 1), :],
                send_sem=sum_send.at[axis, d],
                recv_sem=sum_recv.at[axis, d],
                device_id=peer(axis, d),
                device_id_type=pl.DeviceIdType.MESH,
            )
            for d in range(1, count)
        ]

    x_copies = spread(0, gather_x, gx, ngx)
    for back, at in ((0, TOP_OWN), (8, BOT_OWN)):
        nu, nv = (col_dom.read(f, ITERS, at) for f in (U, V))
        sa, sb, st = (col_dom.read(f, ITERS, at) for f in (A, B, T))
        for blk in range(row_blks):
            values = (
                nv[blk], nu[blk],
                0.5 * (sb[blk] + sa[blk]), 0.5 * (sb[blk] - sa[blk]), 0.5 * st[blk],
            )
            for i, x in enumerate(values):
                turned[blk, pl.ds((16 * i - back) % LANES, 8), :] = x
    for copy in x_copies:
        copy.start()
    for blk in range(row_blks):
        packed[0, pl.ds(blk * LANES, LANES), :] = turned[blk].T
    for at, row, good in ((TOP_OWN, 0, sub < 4), (BOT_OWN, nrow - 8, sub >= 4)):
        nu, nv = (row_dom.read(f, ITERS, at) for f in (U, V))
        sa, sb, st = (row_dom.read(f, ITERS, at) for f in (A, B, T))
        for b in range(nblk):
            r, l = pl.ds(row, 8), slice(b * LANES, (b + 1) * LANES)
            for ref, i, x in (
                (out_vel, 0, nu[b]), (out_vel, 1, nv[b]),
                (out_str, 0, 0.5 * (sa[b] + sb[b])), (out_str, 1, 0.5 * (sa[b] - sb[b])), (out_str, 2, 0.5 * st[b]),
            ):
                ref[i, r, l] = jnp.where(good, x, ref[i, r, l])

    def merge(tile, carry):
        r = pl.ds(pl.multiple_of(tile * 8, 8), 8)
        x = packed[0, r, :]
        places = [((out_vel, i) if i < 2 else (out_str, i - 2)) for i in range(5)]
        first, last = slice(0, LANES), slice(ncol - LANES, ncol)
        new = []
        for i, (ref, at) in enumerate(places):
            edge = pltpu.roll(x, LANES - 16 * i, 1) if i else x
            new.append((ref, at, first, jnp.where(lane < 4, edge, ref[at, r, first])))
            new.append((ref, at, last, jnp.where(lane >= LANES - 4, edge, ref[at, r, last])))
        for ref, at, l, value in new:
            ref[at, r, l] = value
        return carry

    lax.fori_loop(0, nrow // 16, merge, 0, unroll=4)
    for copy in x_copies:
        copy.wait()
    gather_y[gy, 0:1, :] = sum(gather_x[i, 0:1, :] for i in range(ngx))
    y_copies = spread(1, gather_y, gy, ngy)
    for copy in y_copies:
        copy.start()
    lax.fori_loop(nrow // 16, nrow // 8, merge, 0, unroll=4)
    for copy in y_copies:
        copy.wait()
    total = sum(gather_y[i, 0:1, :] for i in range(ngy))
    cells = nrow * ngx * ncol * ngy
    low = lax.broadcasted_iota(jnp.int32, (1, LANES), 1) < half
    out_res[0, 0] = jnp.sum(jnp.where(low, total, 0.0)) * (1.0 / cells)
    out_kin[0, 0] = jnp.sum(jnp.where(low, 0.0, total)) * (0.5 * time_step / 4.0 / cells)


def store_kernel(vel, stress, residual, kinetic, out_vel, out_str, out_res, out_kin, sem):
    copies = [pltpu.make_async_copy(vel.at[i], out_vel.at[i], sem.at[i]) for i in range(2)]
    copies += [pltpu.make_async_copy(stress.at[i], out_str.at[i], sem.at[2 + i]) for i in range(3)]
    for copy in copies:
        copy.start()
    out_res[0, 0] = residual[0, 0]
    out_kin[0, 0] = kinetic[0, 0]
    for copy in copies:
        copy.wait()


def per_device(velocity, stress, strength, ice_mass, wind_stress, current, ice_mask, open_water):
    nrow, ncol = ice_mass.shape
    nblk = ncol // LANES
    row_blks = nrow // LANES
    pad = nrow + 16
    vmem = pltpu.VMEM
    any_spec = pl.BlockSpec(memory_space=pl.ANY)
    vmem_spec = pl.BlockSpec(memory_space=pltpu.VMEM)
    smem_spec = pl.BlockSpec(memory_space=pltpu.SMEM)
    ngx, ngy = lax.axis_size(GX), lax.axis_size(GY)
    new_velocity, new_stress, residual, kinetic = pl.pallas_call(
        main_kernel,
        out_shape=(
            vmem(velocity.shape, F32),
            vmem(stress.shape, F32),
            jax.ShapeDtypeStruct((1, 1), F32),
            jax.ShapeDtypeStruct((1, 1), F32),
        ),
        in_specs=[any_spec] * 8,
        out_specs=(vmem_spec, vmem_spec, smem_spec, smem_spec),
        scratch_shapes=[
            vmem((2, nblk, pad, LANES), F32),
            vmem((3, nrow, ncol), F32),
            vmem((nrow, ncol), F32),
            vmem((nrow, ncol), F32),
            vmem((2, nrow, ncol), F32),
            vmem((2, nrow, ncol), F32),
            vmem((nrow, ncol), jnp.int32),
            vmem((nrow, ncol), jnp.int32),
        ]
        + [vmem((2, nblk, pad, LANES), F32)] * ITERS
        + [vmem((3, nblk, pad, LANES), F32)] * (ITERS + 1)
        + [
            vmem((FIELDS - PR, nblk, pad, LANES), F32),
            vmem((2, nrow + LANES, LANES), F32),
            vmem((FIELDS, nblk, STRIP_ROWS, LANES), F32),
            vmem((ITERS, 2, nblk, STRIP_ROWS, LANES), F32),
            vmem((ITERS, 3, nblk, STRIP_ROWS, LANES), F32),
            vmem((FIELDS, row_blks + 1, STRIP_ROWS, LANES), F32),
            vmem((ITERS, 2, row_blks + 1, STRIP_ROWS, LANES), F32),
            vmem((ITERS, 3, row_blks + 1, STRIP_ROWS, LANES), F32),
            vmem((row_blks, LANES, LANES), F32),
            vmem((ngx, 8, LANES), F32),
            vmem((ngy, 8, LANES), F32),
            pltpu.SemaphoreType.DMA((nblk + 7, CHUNKS)),
            pltpu.SemaphoreType.DMA((2, 2)),
            pltpu.SemaphoreType.DMA((2, 2)),
            pltpu.SemaphoreType.DMA((2, max(ngx, ngy))),
            pltpu.SemaphoreType.DMA((2, max(ngx, ngy))),
        ],
        compiler_params=pltpu.CompilerParams(
            collective_id=0, has_side_effects=True, vmem_limit_bytes=57 * 1024 * 1024
        ),
        name="subcycles",
    )(velocity, stress, strength, ice_mass, wind_stress, current, ice_mask, open_water)
    new_velocity, new_stress, residual, kinetic = pl.pallas_call(
        store_kernel,
        out_shape=(
            jax.ShapeDtypeStruct(velocity.shape, F32),
            jax.ShapeDtypeStruct(stress.shape, F32),
            jax.ShapeDtypeStruct((1, 1), F32),
            jax.ShapeDtypeStruct((1, 1), F32),
        ),
        in_specs=[vmem_spec, vmem_spec, smem_spec, smem_spec],
        out_specs=(any_spec, any_spec, smem_spec, smem_spec),
        scratch_shapes=[pltpu.SemaphoreType.DMA((5,))],
        compiler_params=pltpu.CompilerParams(vmem_limit_bytes=1024 * 1024),
        name="store",
    )(new_velocity, new_stress, residual, kinetic)
    return new_velocity, new_stress, residual.reshape(()), kinetic.reshape(())


def solution(mesh):
    split = Mesh(mesh.devices.reshape(4, 2, 2, 4, 2), AXES)
    return jax.shard_map(
        per_device,
        mesh=split,
        in_specs=(
            P(None, GX, GY),
            P(None, GX, GY),
            P(GX, GY),
            P(GX, GY),
            P(None, GX, GY),
            P(None, GX, GY),
            P(GX, GY),
            P(GX, GY),
        ),
        out_specs=(P(None, GX, GY), P(None, GX, GY), P(), P()),
        check_vma=False,
    )
```

```python
import functools

import jax
import jax.numpy as jnp
from jax import lax
from jax.experimental import pallas as pl
from jax.experimental.pallas import tpu as pltpu
from jax.sharding import Mesh
from jax.sharding import PartitionSpec as P

ITERS = 4
GX = ("gx_0", "gx_1")
GY = ("gy_0", "gy_1", "gy_2")
AXES = GX + GY

relax_rate = 0.8
ecc_square = 4.0
delta_floor = 0.05
time_step = 0.5
drag_coef = 1.0
coriolis = 0.3

F32 = jnp.float32
LANES = 128
CHUNKS = 8
AHEAD = 3
MIDWAY = 3
TALL = 16
FIELDS = 11
U, V, A, B, T, PR, AL, BE, IN, KU, KV = range(FIELDS)
SWAPPED = (V, U, B, A, T, PR, AL, BE, IN, KV, KU)
SPLIT = 6
STRIP_ROWS = 40
TOP_HALO, TOP_OWN, BOT_OWN, BOT_HALO = 8, 12, 20, 28

DECAY = 1.0 / (1.0 + relax_rate)
FLOOR = 4.0 * delta_floor * delta_floor


def lane_ids(height=8):
    return lax.broadcasted_iota(jnp.int32, (height, LANES), 1)


def row_ids(height=8):
    return lax.broadcasted_iota(jnp.int32, (height, LANES), 0)


def from_left(blocks):
    first = lane_ids(blocks[0].shape[0]) == 0
    rolled = [pltpu.roll(x, 1, 1) for x in blocks]
    return [jnp.where(first, rolled[b - 1], rolled[b]) for b in range(len(blocks))]


def from_right(blocks):
    last = lane_ids(blocks[0].shape[0]) == LANES - 1
    rolled = [pltpu.roll(x, LANES - 1, 1) for x in blocks]
    count = len(blocks)
    return [jnp.where(last, rolled[(b + 1) % count], rolled[b]) for b in range(count)]


class Domain:
    def __init__(self, blocks, get, height=8):
        self.blocks = blocks
        self.height = height
        self.get = get

    def read(self, field, level, row):
        ref = self.get(field, level)
        return [ref[b, pl.ds(row, self.height), :] for b in range(self.blocks)]

    def write(self, field, level, row, values):
        ref = self.get(field, level)
        for b in range(self.blocks):
            ref[b, pl.ds(row, self.height), :] = values[b]


def stress_phase(dom, level, row):
    n = dom.blocks
    u, um = dom.read(U, level, row), dom.read(U, level, row - 1)
    v, vm = dom.read(V, level, row), dom.read(V, level, row - 1)
    pr = dom.read(PR, 0, row)
    sa, sb, st = (dom.read(f, level, row) for f in (A, B, T))
    m1, m2, m3, m4 = [], [], [], []
    for b in range(n):
        du, su = u[b] - um[b], u[b] + um[b]
        dv, sv = v[b] - vm[b], v[b] + vm[b]
        m1.append(du + sv)
        m2.append(du - sv)
        m3.append(su + dv)
        m4.append(su - dv)
    l1, l2, l4 = from_left(m1), from_left(m2), from_left(m4)
    na, nb, nt = [], [], []
    for b in range(n):
        div = m1[b] + l2[b]
        ten = m2[b] + l1[b]
        she = m3[b] - l4[b]
        ten4, she4 = 0.25 * ten, 0.25 * she
        rate = lax.rsqrt((div * div + FLOOR) + (ten * ten4 + she * she4))
        vis = pr[b] * rate
        e1 = vis * div - pr[b]
        e2 = vis * ten4
        na.append(DECAY * sa[b] + (e1 + e2))
        nb.append(DECAY * sb[b] + (e1 - e2))
        nt.append(DECAY * st[b] + vis * she4)
    dom.write(A, level + 1, row, na)
    dom.write(B, level + 1, row, nb)
    dom.write(T, level + 1, row, nt)
    return na, nb, nt


def velocity_phase(dom, level, row):
    n = dom.blocks
    sa, sap = dom.read(A, level + 1, row), dom.read(A, level + 1, row + 1)
    sb, sbp = dom.read(B, level + 1, row), dom.read(B, level + 1, row + 1)
    st, stp = dom.read(T, level + 1, row), dom.read(T, level + 1, row + 1)
    e, g, h, j = [], [], [], []
    for b in range(n):
        da, sumt = sap[b] - sa[b], stp[b] + st[b]
        dt, sumb = stp[b] - st[b], sbp[b] + sb[b]
        e.append(da + sumt)
        g.append(da - sumt)
        h.append(dt + sumb)
        j.append(dt - sumb)
    re, rh = from_right(e), from_right(h)
    u, v = dom.read(U, level, row), dom.read(V, level, row)
    al, be, inert = (dom.read(f, 0, row) for f in (AL, BE, IN))
    ku, kv = dom.read(KU, 0, row), dom.read(KV, 0, row)
    nu, nv = [], []
    for b in range(n):
        ru = inert[b] * u[b] + (re[b] + g[b]) + ku[b]
        rv = inert[b] * v[b] + (rh[b] + j[b]) + kv[b]
        nu.append(al[b] * ru + be[b] * rv)
        nv.append(al[b] * rv - be[b] * ru)
    dom.write(U, level + 1, row, nu)
    dom.write(V, level + 1, row, nv)
    return u, v, nu, nv, inert


def square_sums(phase, keep):
    res, kin = None, None
    for u, v, nu, nv, inert, mask in zip(*phase, keep):
        if mask is False:
            continue
        du, dv = nu - u, nv - v
        r = du * du + dv * dv
        k = inert * (nu * nu + nv * nv)
        if mask is not None:
            r, k = jnp.where(mask, r, 0.0), jnp.where(mask, k, 0.0)
        res = r if res is None else res + r
        kin = k if kin is None else kin + k
    return res, kin


def wavefront(tiles, phases, carry, arrive=None, group=1, midway=None):
    depth = max(lag for lag, _ in phases)

    def step(t, carry, active):
        for lag, phase in active:
            carry = phase(t - lag, carry)
        return carry

    def steady(t, carry):
        return step(t, carry, phases)

    for t in range(depth):
        if arrive is not None and t % group == 0:
            arrive(t // group)
        carry = step(t, carry, [p for p in phases if p[0] <= t])
    if arrive is None:
        carry = lax.fori_loop(depth, tiles, steady, carry)
    else:
        whole = -(-depth // group)
        if depth < whole * group:
            carry = lax.fori_loop(depth, whole * group, steady, carry)

        def run_group(c, carry):
            arrive(c)
            return lax.fori_loop(c * group, (c + 1) * group, steady, carry)

        middle = max(whole, MIDWAY)
        carry = lax.fori_loop(whole, middle, run_group, carry)
        midway()
        carry = lax.fori_loop(middle, tiles // group, run_group, carry)
    for t in range(tiles, tiles + depth):
        carry = step(t, carry, [p for p in phases if t - p[0] < tiles])
    return carry


def main_kernel(
    vel, stress, strength, mass, wind, current, mask, water,
    out_vel, out_str, out_sum,
    uv0, str_in, strength_in, mass_in, wind_in, cur_in, mask_in, water_in,
    uv1, uv2, uv3, uv4, s0, s1, s2, s3, s4, coef,
    packed, rows0, rows_uv, rows_s, cols0, cols_uv, cols_s, turned,
    gather_x, gather_y, in_sem, send_sem, recv_sem, sum_send, sum_recv,
):
    nrow, ncol = mass.shape
    nblk = ncol // LANES
    tiles = nrow // TALL
    per = nrow // CHUNKS
    row_blks = nrow // LANES
    gx, gy = lax.axis_index(GX), lax.axis_index(GY)
    ngx, ngy = lax.axis_size(GX), lax.axis_size(GY)

    def copies(c):
        r = pl.ds(c * per, per)
        out = []
        for b in range(nblk):
            out.append((vel.at[:, r, b * LANES : (b + 1) * LANES], uv0.at[:, b, pl.ds(c * per + 8, per), :]))
        for src, dst in ((stress, str_in), (wind, wind_in), (current, cur_in)):
            out.append((src.at[:, r, :], dst.at[:, r, :]))
        for src, dst in ((strength, strength_in), (mass, mass_in), (mask, mask_in), (water, water_in)):
            out.append((src.at[r, :], dst.at[r, :]))
        slot = AHEAD if isinstance(c, int) and c == CHUNKS - 1 else lax.rem(c, AHEAD)
        return [pltpu.make_async_copy(s, d, in_sem.at[i, slot]) for i, (s, d) in enumerate(out)]

    for c in list(range(AHEAD)) + [CHUNKS - 1]:
        for copy in copies(c):
            copy.start()

    def peer(axis, step):
        if axis == 0:
            x, y = lax.rem(gx + step + ngx, ngx), gy
        else:
            x, y = gx, lax.rem(gy + step + ngy, ngy)
        ids = {}
        for names, index in ((GX, x), (GY, y)):
            for name in reversed(names):
                size = lax.axis_size(name)
                ids[name] = lax.rem(index, size)
                index = lax.div(index, size)
        return tuple(ids[name] for name in AXES)

    barrier = pltpu.get_barrier_semaphore()
    for axis, count in ((0, ngx), (1, ngy)):
        for step in range(1, count):
            pl.semaphore_signal(barrier, 1, device_id=peer(axis, step), device_id_type=pl.DeviceIdType.MESH)

    def prologue(row, b, height):
        r, l = pl.ds(row, height), slice(b * LANES, (b + 1) * LANES)
        ice = mask_in[r, l] > water_in[r, l]
        m = mass_in[r, l]
        diag, turn = m * (1.0 / time_step) + drag_coef, m * coriolis
        inv = jnp.where(ice, 0.25 / (diag * diag + turn * turn), 0.0)
        first, second = str_in[0, r, l], str_in[1, r, l]
        pres = jnp.where(ice, strength_in[r, l] * (relax_rate * DECAY), 0.0)
        at = pl.ds(row + 8, height)
        return [
            uv0[0, b, at, :], uv0[1, b, at, :],
            first + second, first - second, 2.0 * str_in[2, r, l],
            pres, diag * inv, turn * inv, m * (4.0 / time_step),
            4.0 * (wind_in[0, r, l] + drag_coef * cur_in[0, r, l]),
            4.0 * (wind_in[1, r, l] + drag_coef * cur_in[1, r, l]),
        ]

    def exchange(strip, axis):
        out = []
        for way, (step, src, dst) in enumerate(((-1, TOP_OWN, BOT_HALO), (1, BOT_OWN + 4, TOP_HALO))):
            out.append(
                pltpu.make_async_remote_copy(
                    src_ref=strip.at[:, :, pl.ds(src, 4), :],
                    dst_ref=strip.at[:, :, pl.ds(dst, 4), :],
                    send_sem=send_sem.at[axis, way],
                    recv_sem=recv_sem.at[axis, way],
                    device_id=peer(axis, step),
                    device_id_type=pl.DeviceIdType.MESH,
                )
            )
        return out

    def no_outside(strip, index, count):
        @pl.when(index == 0)
        def _():
            strip[:, :, TOP_HALO : TOP_HALO + 4, :] = jnp.zeros(strip.shape[:2] + (4, LANES), F32)

        @pl.when(index == count - 1)
        def _():
            strip[:, :, BOT_HALO : BOT_HALO + 4, :] = jnp.zeros(strip.shape[:2] + (4, LANES), F32)

    row_copies = exchange(rows0, 0)

    def send_rows():
        for copy in copies(CHUNKS - 1):
            copy.wait()
        for row, at in ((0, TOP_OWN), (nrow - 8, BOT_OWN)):
            for b in range(nblk):
                for f, x in enumerate(prologue(row, b, 8)):
                    rows0[f, b, pl.ds(at, 8), :] = x
        pl.semaphore_wait(barrier, ngx + ngy - 2)
        for copy in row_copies:
            copy.start()

    uvs, ss = (uv0, uv1, uv2, uv3, uv4), (s0, s1, s2, s3, s4)

    def main_get(field, level):
        if field in (U, V):
            return uvs[level].at[field]
        if field in (A, B, T):
            return ss[level].at[field - A]
        return coef.at[field - PR]

    main = Domain(nblk, main_get, TALL)
    lane = lane_ids()
    tall_lane = lane_ids(TALL)

    def pack(first, last):
        lanes = lane_ids(first[0].shape[0])
        out = []
        for names in (SWAPPED[:SPLIT], SWAPPED[SPLIT:]):
            edges = [jnp.where(lanes < LANES // 2, first[f], last[f]) for f in names]
            total = pltpu.roll(edges[1], 16, 1)
            for q in range(2, len(edges)):
                total = jnp.where(lanes < 16 * q - 8, total, pltpu.roll(edges[q], 16 * q, 1))
            out.append(jnp.where((lanes < 8) | (lanes >= LANES - 8), edges[0], total))
        return out

    def arrive(c):
        if isinstance(c, int):
            if c < CHUNKS - 1:
                for copy in copies(c):
                    copy.wait()
            if c + AHEAD < CHUNKS - 1:
                for copy in copies(c + AHEAD):
                    copy.start()
        else:

            @pl.when(c < CHUNKS - 1)
            def _():
                for copy in copies(c):
                    copy.wait()

            @pl.when(c < CHUNKS - 1 - AHEAD)
            def _():
                for copy in copies(c + AHEAD):
                    copy.start()

    def prepare(tile, carry):
        row = tile * TALL if isinstance(tile, int) else pl.multiple_of(tile * TALL, 8)
        at = row + 8
        edges = []
        for b in range(nblk):
            fields = prologue(row, b, TALL)
            for f in (A, B, T):
                s0[f - A, b, pl.ds(at, TALL), :] = fields[f]
            for f in range(PR, FIELDS):
                coef[f - PR, b, pl.ds(at, TALL), :] = fields[f]
            if b in (0, nblk - 1):
                edges.append(fields)
        for i, x in enumerate(pack(edges[0], edges[-1])):
            packed[i, pl.ds(row, TALL), :] = x
        return carry

    def at_row(tile):
        return tile * TALL + 8 if isinstance(tile, int) else pl.multiple_of(tile * TALL + 8, 8)

    def stress_at(level):
        def phase(tile, carry):
            stress_phase(main, level, at_row(tile))
            return carry

        return phase

    def velocity_at(level):
        def phase(tile, carry):
            velocity_phase(main, level, at_row(tile))
            return carry

        return phase

    def put_stress(tile, blocks):
        na, nb, nt = blocks
        r = pl.ds(at_row(tile) - 8, TALL)
        for b in range(nblk):
            l = slice(b * LANES, (b + 1) * LANES)
            out_str[0, r, l] = 0.5 * (na[b] + nb[b])
            out_str[1, r, l] = 0.5 * (na[b] - nb[b])
            out_str[2, r, l] = 0.5 * nt[b]

    def last_stress(tile, carry):
        put_stress(tile, stress_phase(main, ITERS - 1, at_row(tile)))
        return carry

    tall_inner = [None] * nblk
    tall_inner[0] = tall_lane >= 4
    tall_inner[nblk - 1] = tall_lane < LANES - 4

    def last_velocity(tile, carry):
        u, v, nu, nv, inert = velocity_phase(main, ITERS - 1, at_row(tile))
        r = pl.ds(at_row(tile) - 8, TALL)
        for b in range(nblk):
            l = slice(b * LANES, (b + 1) * LANES)
            out_vel[0, r, l] = nu[b]
            out_vel[1, r, l] = nv[b]
        res, kin = square_sums((u, v, nu, nv, inert), tall_inner)
        keep = row_ids(TALL) + tile * TALL
        good = (keep >= 4) & (keep < nrow - 4)
        return carry[0] + jnp.where(good, res, 0.0), carry[1] + jnp.where(good, kin, 0.0)

    zero = jnp.zeros((TALL, LANES), F32)
    wavefront(
        tiles,
        [(8, velocity_at(1)), (6, stress_at(1)), (4, velocity_at(0)), (2, stress_at(0)), (0, prepare)],
        0,
        arrive,
        per // TALL,
        send_rows,
    )

    for copy in row_copies:
        copy.wait()
    no_outside(rows0, gx, ngx)
    for at, to in ((BOT_HALO, nrow), (TOP_HALO - 4, nrow + LANES - 8)):
        ends = [[rows0[f, b, pl.ds(at, 8), :] for f in range(FIELDS)] for b in (0, nblk - 1)]
        for i, x in enumerate(pack(*ends)):
            packed[i, pl.ds(to, 8), :] = x
    for i, names in enumerate((range(SPLIT), range(SPLIT, FIELDS))):
        for blk in range(row_blks + 1):
            flat = packed[i, pl.ds(blk * LANES, LANES), :].T
            for q, f in enumerate(names):
                for at, to in ((16 * q, TOP_OWN), ((16 * q - 8) % LANES, BOT_OWN)):
                    x = flat[at : at + 8, :]
                    cols0[f, blk, pl.ds(to, 8), :] = -x if f == BE else x
    col_copies = exchange(cols0, 1)
    for copy in col_copies:
        copy.start()

    sums = wavefront(
        tiles,
        [(6, last_velocity), (4, last_stress), (2, velocity_at(2)), (0, stress_at(2))],
        (zero, zero),
    )

    def strip_get(first, uv, s):
        def get(field, level):
            if level == 0:
                return first.at[field]
            return uv.at[level - 1, field] if field in (U, V) else s.at[level - 1, field - A]

        return get

    for copy in col_copies:
        copy.wait()
    no_outside(cols0, gy, ngy)
    row_dom = Domain(nblk, strip_get(rows0, rows_uv, rows_s))
    col_dom = Domain(row_blks + 1, strip_get(cols0, cols_uv, cols_s))
    row_ends, col_ends = {}, {}
    for level in range(ITERS):
        for at in (8, 16, 24):
            stress_phase(row_dom, level, at)
            stress_phase(col_dom, level, at)
        for at in (8, 16, 24) if level < ITERS - 1 else (8, 24):
            row_ends[at] = velocity_phase(row_dom, level, at)
            col_ends[at] = velocity_phase(col_dom, level, at)

    def add(sums, more):
        return sums[0] + more[0], sums[1] + more[1]

    sub = row_ids()
    sums = [sum(x[8 * i : 8 * i + 8] for i in range(TALL // 8)) for x in sums]
    inner = [None] * nblk
    inner[0] = lane >= 4
    inner[nblk - 1] = lane < LANES - 4
    for at, good in ((8, sub >= 4), (24, sub < 4)):
        sums = add(sums, square_sums(row_ends[at], [good if m is None else good & m for m in inner]))
        sums = add(sums, square_sums(col_ends[at], [good] * row_blks + [False]))

    half = LANES // 2
    both = [x + pltpu.roll(x, half, 1) for x in sums]
    mine = jnp.where(lane < half, both[0], both[1])
    gather_x[gx, 0:1, :] = jnp.sum(mine, axis=0, keepdims=True)

    def spread(axis, slots, me, count):
        return [
            pltpu.make_async_remote_copy(
                src_ref=slots.at[me, pl.ds(0, 1), :],
                dst_ref=slots.at[me, pl.ds(0, 1), :],
                send_sem=sum_send.at[axis * ngx + d],
                recv_sem=sum_recv.at[axis * ngx + d],
                device_id=peer(axis, d),
                device_id_type=pl.DeviceIdType.MESH,
            )
            for d in range(1, count)
        ]

    x_copies = spread(0, gather_x, gx, ngx)
    for back, at in ((0, TOP_OWN), (8, BOT_OWN)):
        nu, nv = (col_dom.read(f, ITERS, at) for f in (U, V))
        sa, sb, st = (col_dom.read(f, ITERS, at) for f in (A, B, T))
        for blk in range(row_blks):
            values = (
                nv[blk], nu[blk],
                0.5 * (sb[blk] + sa[blk]), 0.5 * (sb[blk] - sa[blk]), 0.5 * st[blk],
            )
            for i, x in enumerate(values):
                turned[blk, pl.ds((16 * i - back) % LANES, 8), :] = x
    for copy in x_copies:
        copy.start()
    for blk in range(row_blks):
        packed[0, pl.ds(blk * LANES, LANES), :] = turned[blk].T
    for at, row, good in ((TOP_OWN, 0, sub < 4), (BOT_OWN, nrow - 8, sub >= 4)):
        nu, nv = (row_dom.read(f, ITERS, at) for f in (U, V))
        sa, sb, st = (row_dom.read(f, ITERS, at) for f in (A, B, T))
        for b in range(nblk):
            r, l = pl.ds(row, 8), slice(b * LANES, (b + 1) * LANES)
            for ref, i, x in (
                (out_vel, 0, nu[b]), (out_vel, 1, nv[b]),
                (out_str, 0, 0.5 * (sa[b] + sb[b])), (out_str, 1, 0.5 * (sa[b] - sb[b])), (out_str, 2, 0.5 * st[b]),
            ):
                ref[i, r, l] = jnp.where(good, x, ref[i, r, l])

    def merge(tile, carry):
        r = pl.ds(pl.multiple_of(tile * 8, 8), 8)
        x = packed[0, r, :]
        places = [((out_vel, i) if i < 2 else (out_str, i - 2)) for i in range(5)]
        first, last = slice(0, LANES), slice(ncol - LANES, ncol)
        new = []
        for i, (ref, at) in enumerate(places):
            edge = pltpu.roll(x, LANES - 16 * i, 1) if i else x
            new.append((ref, at, first, jnp.where(lane < 4, edge, ref[at, r, first])))
            new.append((ref, at, last, jnp.where(lane >= LANES - 4, edge, ref[at, r, last])))
        for ref, at, l, value in new:
            ref[at, r, l] = value
        return carry

    lax.fori_loop(0, nrow // 16, merge, 0, unroll=4)
    for copy in x_copies:
        copy.wait()
    gather_y[gy, 0:1, :] = sum(gather_x[i, 0:1, :] for i in range(ngx))
    y_copies = spread(1, gather_y, gy, ngy)
    for copy in y_copies:
        copy.start()
    lax.fori_loop(nrow // 16, nrow // 8, merge, 0, unroll=4)
    for copy in y_copies:
        copy.wait()
    out_sum[...] = sum(gather_y[i, 0:1, :] for i in range(ngy))


def store_kernel(cells, vel, stress, total, out_vel, out_str, out_res, out_kin, res, kin, sem):
    copies = [pltpu.make_async_copy(vel.at[i], out_vel.at[i], sem.at[i]) for i in range(2)]
    copies += [pltpu.make_async_copy(stress.at[i], out_str.at[i], sem.at[2 + i]) for i in range(3)]
    low = lax.broadcasted_iota(jnp.int32, (1, LANES), 1) < LANES // 2
    both = total[...]
    res[...] = jnp.sum(jnp.where(low, both, 0.0), axis=1, keepdims=True) * (1.0 / cells)
    kin[...] = jnp.sum(jnp.where(low, 0.0, both), axis=1, keepdims=True) * (0.5 * time_step / 4.0 / cells)
    copies += [pltpu.make_async_copy(res, out_res, sem.at[5]), pltpu.make_async_copy(kin, out_kin, sem.at[6])]
    for copy in copies:
        copy.start()
    for copy in copies:
        copy.wait()


def per_device(velocity, stress, strength, ice_mass, wind_stress, current, ice_mask, open_water):
    nrow, ncol = ice_mass.shape
    nblk = ncol // LANES
    row_blks = nrow // LANES
    pad = nrow + 16
    vmem = pltpu.VMEM
    any_spec = pl.BlockSpec(memory_space=pl.ANY)
    vmem_spec = pl.BlockSpec(memory_space=pltpu.VMEM)
    ngx, ngy = lax.axis_size(GX), lax.axis_size(GY)
    new_velocity, new_stress, total = pl.pallas_call(
        main_kernel,
        out_shape=(
            vmem(velocity.shape, F32),
            vmem(stress.shape, F32),
            vmem((1, LANES), F32),
        ),
        in_specs=[any_spec] * 8,
        out_specs=(vmem_spec, vmem_spec, vmem_spec),
        scratch_shapes=[
            vmem((2, nblk, pad, LANES), F32),
            vmem((3, nrow, ncol), F32),
            vmem((nrow, ncol), F32),
            vmem((nrow, ncol), F32),
            vmem((2, nrow, ncol), F32),
            vmem((2, nrow, ncol), F32),
            vmem((nrow, ncol), jnp.int32),
            vmem((nrow, ncol), jnp.int32),
        ]
        + [vmem((2, nblk, pad, LANES), F32)] * ITERS
        + [vmem((3, nblk, pad, LANES), F32)] * (ITERS + 1)
        + [
            vmem((FIELDS - PR, nblk, pad, LANES), F32),
            vmem((2, nrow + LANES, LANES), F32),
            vmem((FIELDS, nblk, STRIP_ROWS, LANES), F32),
            vmem((ITERS, 2, nblk, STRIP_ROWS, LANES), F32),
            vmem((ITERS, 3, nblk, STRIP_ROWS, LANES), F32),
            vmem((FIELDS, row_blks + 1, STRIP_ROWS, LANES), F32),
            vmem((ITERS, 2, row_blks + 1, STRIP_ROWS, LANES), F32),
            vmem((ITERS, 3, row_blks + 1, STRIP_ROWS, LANES), F32),
            vmem((row_blks, LANES, LANES), F32),
            vmem((ngx, 8, LANES), F32),
            vmem((ngy, 8, LANES), F32),
            pltpu.SemaphoreType.DMA((nblk + 7, AHEAD + 1)),
            pltpu.SemaphoreType.DMA((2, 2)),
            pltpu.SemaphoreType.DMA((2, 2)),
            pltpu.SemaphoreType.DMA((ngx + ngy,)),
            pltpu.SemaphoreType.DMA((ngx + ngy,)),
        ],
        compiler_params=pltpu.CompilerParams(
            collective_id=0, has_side_effects=True, vmem_limit_bytes=57 * 1024 * 1024
        ),
        name="subcycles",
    )(velocity, stress, strength, ice_mass, wind_stress, current, ice_mask, open_water)
    new_velocity, new_stress, residual, kinetic = pl.pallas_call(
        functools.partial(store_kernel, nrow * ngx * ncol * ngy),
        out_shape=(
            jax.ShapeDtypeStruct(velocity.shape, F32),
            jax.ShapeDtypeStruct(stress.shape, F32),
            jax.ShapeDtypeStruct((1, 1), F32),
            jax.ShapeDtypeStruct((1, 1), F32),
        ),
        in_specs=[vmem_spec] * 3,
        out_specs=(any_spec,) * 4,
        scratch_shapes=[vmem((1, 1), F32), vmem((1, 1), F32), pltpu.SemaphoreType.DMA((7,))],
        compiler_params=pltpu.CompilerParams(vmem_limit_bytes=1024 * 1024),
        name="store",
    )(new_velocity, new_stress, total)
    return new_velocity, new_stress, residual.reshape(()), kinetic.reshape(())


def solution(mesh):
    split = Mesh(mesh.devices.reshape(4, 2, 2, 4, 2), AXES)
    return jax.shard_map(
        per_device,
        mesh=split,
        in_specs=(
            P(None, GX, GY),
            P(None, GX, GY),
            P(GX, GY),
            P(GX, GY),
            P(None, GX, GY),
            P(None, GX, GY),
            P(GX, GY),
            P(GX, GY),
        ),
        out_specs=(P(None, GX, GY), P(None, GX, GY), P(), P()),
        check_vma=False,
    )
```

```python
import functools

import jax
import jax.numpy as jnp
from jax import lax
from jax.experimental import pallas as pl
from jax.experimental.pallas import tpu as pltpu
from jax.sharding import Mesh
from jax.sharding import PartitionSpec as P

ITERS = 4
GX = ("gx_0", "gx_1")
GY = ("gy_0", "gy_1", "gy_2")
AXES = GX + GY

relax_rate = 0.8
ecc_square = 4.0
delta_floor = 0.05
time_step = 0.5
drag_coef = 1.0
coriolis = 0.3

F32 = jnp.float32
LANES = 128
CHUNKS = 8
AHEAD = 3
MIDWAY = 3
TALL = 32
FIELDS = 11
U, V, A, B, T, PR, AL, BE, IN, KU, KV = range(FIELDS)
SWAPPED = (V, U, B, A, T, PR, AL, BE, IN, KV, KU)
SPLIT = 6
STRIP_ROWS = 40
TOP_HALO, TOP_OWN, BOT_OWN, BOT_HALO = 8, 12, 20, 28

DECAY = 1.0 / (1.0 + relax_rate)
FLOOR = 4.0 * delta_floor * delta_floor


def lane_ids(height=8):
    return lax.broadcasted_iota(jnp.int32, (height, LANES), 1)


def row_ids(height=8):
    return lax.broadcasted_iota(jnp.int32, (height, LANES), 0)


def from_left(blocks):
    first = lane_ids(blocks[0].shape[0]) == 0
    rolled = [pltpu.roll(x, 1, 1) for x in blocks]
    return [jnp.where(first, rolled[b - 1], rolled[b]) for b in range(len(blocks))]


def from_right(blocks):
    last = lane_ids(blocks[0].shape[0]) == LANES - 1
    rolled = [pltpu.roll(x, LANES - 1, 1) for x in blocks]
    count = len(blocks)
    return [jnp.where(last, rolled[(b + 1) % count], rolled[b]) for b in range(count)]


class Domain:
    def __init__(self, blocks, get, height=8):
        self.blocks = blocks
        self.height = height
        self.get = get

    def read(self, field, level, row):
        ref = self.get(field, level)
        return [ref[b, pl.ds(row, self.height), :] for b in range(self.blocks)]

    def write(self, field, level, row, values):
        ref = self.get(field, level)
        for b in range(self.blocks):
            ref[b, pl.ds(row, self.height), :] = values[b]


def stress_phase(dom, level, row):
    n = dom.blocks
    u, um = dom.read(U, level, row), dom.read(U, level, row - 1)
    v, vm = dom.read(V, level, row), dom.read(V, level, row - 1)
    pr = dom.read(PR, 0, row)
    sa, sb, st = (dom.read(f, level, row) for f in (A, B, T))
    m1, m2, m3, m4 = [], [], [], []
    for b in range(n):
        du, su = u[b] - um[b], u[b] + um[b]
        dv, sv = v[b] - vm[b], v[b] + vm[b]
        m1.append(du + sv)
        m2.append(du - sv)
        m3.append(su + dv)
        m4.append(su - dv)
    l1, l2, l4 = from_left(m1), from_left(m2), from_left(m4)
    na, nb, nt = [], [], []
    for b in range(n):
        div = m1[b] + l2[b]
        ten = m2[b] + l1[b]
        she = m3[b] - l4[b]
        ten4, she4 = 0.25 * ten, 0.25 * she
        rate = lax.rsqrt((div * div + FLOOR) + (ten * ten4 + she * she4))
        vis = pr[b] * rate
        e1 = vis * div - pr[b]
        e2 = vis * ten4
        na.append(DECAY * sa[b] + (e1 + e2))
        nb.append(DECAY * sb[b] + (e1 - e2))
        nt.append(DECAY * st[b] + vis * she4)
    dom.write(A, level + 1, row, na)
    dom.write(B, level + 1, row, nb)
    dom.write(T, level + 1, row, nt)
    return na, nb, nt


def velocity_phase(dom, level, row):
    n = dom.blocks
    sa, sap = dom.read(A, level + 1, row), dom.read(A, level + 1, row + 1)
    sb, sbp = dom.read(B, level + 1, row), dom.read(B, level + 1, row + 1)
    st, stp = dom.read(T, level + 1, row), dom.read(T, level + 1, row + 1)
    e, g, h, j = [], [], [], []
    for b in range(n):
        da, sumt = sap[b] - sa[b], stp[b] + st[b]
        dt, sumb = stp[b] - st[b], sbp[b] + sb[b]
        e.append(da + sumt)
        g.append(da - sumt)
        h.append(dt + sumb)
        j.append(dt - sumb)
    re, rh = from_right(e), from_right(h)
    u, v = dom.read(U, level, row), dom.read(V, level, row)
    al, be, inert = (dom.read(f, 0, row) for f in (AL, BE, IN))
    ku, kv = dom.read(KU, 0, row), dom.read(KV, 0, row)
    nu, nv = [], []
    for b in range(n):
        ru = inert[b] * u[b] + (re[b] + g[b]) + ku[b]
        rv = inert[b] * v[b] + (rh[b] + j[b]) + kv[b]
        nu.append(al[b] * ru + be[b] * rv)
        nv.append(al[b] * rv - be[b] * ru)
    dom.write(U, level + 1, row, nu)
    dom.write(V, level + 1, row, nv)
    return u, v, nu, nv, inert


def square_sums(phase, keep):
    res, kin = None, None
    for u, v, nu, nv, inert, mask in zip(*phase, keep):
        if mask is False:
            continue
        du, dv = nu - u, nv - v
        r = du * du + dv * dv
        k = inert * (nu * nu + nv * nv)
        if mask is not None:
            r, k = jnp.where(mask, r, 0.0), jnp.where(mask, k, 0.0)
        res = r if res is None else res + r
        kin = k if kin is None else kin + k
    return res, kin


def wavefront(tiles, phases, carry, arrive=None, group=1, midway=None):
    depth = max(lag for lag, _ in phases)

    def step(t, carry, active):
        for lag, phase in active:
            carry = phase(t - lag, carry)
        return carry

    def steady(t, carry):
        return step(t, carry, phases)

    for t in range(depth):
        if arrive is not None and t % group == 0:
            arrive(t // group)
        carry = step(t, carry, [p for p in phases if p[0] <= t])
    if arrive is None:
        carry = lax.fori_loop(depth, tiles, steady, carry)
    else:
        whole = -(-depth // group)
        if depth < whole * group:
            carry = lax.fori_loop(depth, whole * group, steady, carry)

        def run_group(c, carry):
            arrive(c)
            return lax.fori_loop(c * group, (c + 1) * group, steady, carry)

        middle = max(whole, MIDWAY)
        carry = lax.fori_loop(whole, middle, run_group, carry)
        midway()
        carry = lax.fori_loop(middle, tiles // group, run_group, carry)
    for t in range(tiles, tiles + depth):
        carry = step(t, carry, [p for p in phases if t - p[0] < tiles])
    return carry


def main_kernel(
    vel, stress, strength, mass, wind, current, mask, water,
    out_vel, out_str, out_sum,
    uv0, str_in, strength_in, mass_in, wind_in, cur_in, mask_in, water_in,
    uv1, uv2, uv3, uv4, s0, s1, s2, s3, s4, coef,
    packed, rows0, rows_uv, rows_s, cols0, cols_uv, cols_s, turned,
    gather_x, gather_y, in_sem, send_sem, recv_sem, sum_send, sum_recv,
):
    nrow, ncol = mass.shape
    nblk = ncol // LANES
    tiles = nrow // TALL
    per = nrow // CHUNKS
    row_blks = nrow // LANES
    gx, gy = lax.axis_index(GX), lax.axis_index(GY)
    ngx, ngy = lax.axis_size(GX), lax.axis_size(GY)

    def copies(c):
        r = pl.ds(c * per, per)
        out = []
        for b in range(nblk):
            out.append((vel.at[:, r, b * LANES : (b + 1) * LANES], uv0.at[:, b, pl.ds(c * per + 8, per), :]))
        for src, dst in ((stress, str_in), (wind, wind_in), (current, cur_in)):
            out.append((src.at[:, r, :], dst.at[:, r, :]))
        for src, dst in ((strength, strength_in), (mass, mass_in), (mask, mask_in), (water, water_in)):
            out.append((src.at[r, :], dst.at[r, :]))
        slot = AHEAD if isinstance(c, int) and c == CHUNKS - 1 else lax.rem(c, AHEAD)
        return [pltpu.make_async_copy(s, d, in_sem.at[i, slot]) for i, (s, d) in enumerate(out)]

    for c in list(range(AHEAD)) + [CHUNKS - 1]:
        for copy in copies(c):
            copy.start()

    def peer(axis, step):
        if axis == 0:
            x, y = lax.rem(gx + step + ngx, ngx), gy
        else:
            x, y = gx, lax.rem(gy + step + ngy, ngy)
        ids = {}
        for names, index in ((GX, x), (GY, y)):
            for name in reversed(names):
                size = lax.axis_size(name)
                ids[name] = lax.rem(index, size)
                index = lax.div(index, size)
        return tuple(ids[name] for name in AXES)

    barrier = pltpu.get_barrier_semaphore()
    for axis, count in ((0, ngx), (1, ngy)):
        for step in range(1, count):
            pl.semaphore_signal(barrier, 1, device_id=peer(axis, step), device_id_type=pl.DeviceIdType.MESH)

    def prologue(row, b, height):
        r, l = pl.ds(row, height), slice(b * LANES, (b + 1) * LANES)
        ice = mask_in[r, l] > water_in[r, l]
        m = mass_in[r, l]
        diag, turn = m * (1.0 / time_step) + drag_coef, m * coriolis
        inv = jnp.where(ice, 0.25 / (diag * diag + turn * turn), 0.0)
        first, second = str_in[0, r, l], str_in[1, r, l]
        pres = jnp.where(ice, strength_in[r, l] * (relax_rate * DECAY), 0.0)
        at = pl.ds(row + 8, height)
        return [
            uv0[0, b, at, :], uv0[1, b, at, :],
            first + second, first - second, 2.0 * str_in[2, r, l],
            pres, diag * inv, turn * inv, m * (4.0 / time_step),
            4.0 * (wind_in[0, r, l] + drag_coef * cur_in[0, r, l]),
            4.0 * (wind_in[1, r, l] + drag_coef * cur_in[1, r, l]),
        ]

    def exchange(strip, axis):
        out = []
        for way, (step, src, dst) in enumerate(((-1, TOP_OWN, BOT_HALO), (1, BOT_OWN + 4, TOP_HALO))):
            out.append(
                pltpu.make_async_remote_copy(
                    src_ref=strip.at[:, :, pl.ds(src, 4), :],
                    dst_ref=strip.at[:, :, pl.ds(dst, 4), :],
                    send_sem=send_sem.at[axis, way],
                    recv_sem=recv_sem.at[axis, way],
                    device_id=peer(axis, step),
                    device_id_type=pl.DeviceIdType.MESH,
                )
            )
        return out

    def no_outside(strip, index, count):
        @pl.when(index == 0)
        def _():
            strip[:, :, TOP_HALO : TOP_HALO + 4, :] = jnp.zeros(strip.shape[:2] + (4, LANES), F32)

        @pl.when(index == count - 1)
        def _():
            strip[:, :, BOT_HALO : BOT_HALO + 4, :] = jnp.zeros(strip.shape[:2] + (4, LANES), F32)

    row_copies = exchange(rows0, 0)

    def send_rows():
        for copy in copies(CHUNKS - 1):
            copy.wait()
        for row, at in ((0, TOP_OWN), (nrow - 8, BOT_OWN)):
            for b in range(nblk):
                for f, x in enumerate(prologue(row, b, 8)):
                    rows0[f, b, pl.ds(at, 8), :] = x
        pl.semaphore_wait(barrier, ngx + ngy - 2)
        for copy in row_copies:
            copy.start()

    uvs, ss = (uv0, uv1, uv2, uv3, uv4), (s0, s1, s2, s3, s4)

    def main_get(field, level):
        if field in (U, V):
            return uvs[level].at[field]
        if field in (A, B, T):
            return ss[level].at[field - A]
        return coef.at[field - PR]

    main = Domain(nblk, main_get, TALL)
    lane = lane_ids()
    tall_lane = lane_ids(TALL)

    def pack(first, last):
        lanes = lane_ids(first[0].shape[0])
        out = []
        for names in (SWAPPED[:SPLIT], SWAPPED[SPLIT:]):
            edges = [jnp.where(lanes < LANES // 2, first[f], last[f]) for f in names]
            total = pltpu.roll(edges[1], 16, 1)
            for q in range(2, len(edges)):
                total = jnp.where(lanes < 16 * q - 8, total, pltpu.roll(edges[q], 16 * q, 1))
            out.append(jnp.where((lanes < 8) | (lanes >= LANES - 8), edges[0], total))
        return out

    def arrive(c):
        if isinstance(c, int):
            if c < CHUNKS - 1:
                for copy in copies(c):
                    copy.wait()
            if c + AHEAD < CHUNKS - 1:
                for copy in copies(c + AHEAD):
                    copy.start()
        else:

            @pl.when(c < CHUNKS - 1)
            def _():
                for copy in copies(c):
                    copy.wait()

            @pl.when(c < CHUNKS - 1 - AHEAD)
            def _():
                for copy in copies(c + AHEAD):
                    copy.start()

    def prepare(tile, carry):
        row = tile * TALL if isinstance(tile, int) else pl.multiple_of(tile * TALL, 8)
        at = row + 8
        edges = []
        for b in range(nblk):
            fields = prologue(row, b, TALL)
            for f in (A, B, T):
                s0[f - A, b, pl.ds(at, TALL), :] = fields[f]
            for f in range(PR, FIELDS):
                coef[f - PR, b, pl.ds(at, TALL), :] = fields[f]
            if b in (0, nblk - 1):
                edges.append(fields)
        for i, x in enumerate(pack(edges[0], edges[-1])):
            packed[i, pl.ds(row, TALL), :] = x
        return carry

    def at_row(tile):
        return tile * TALL + 8 if isinstance(tile, int) else pl.multiple_of(tile * TALL + 8, 8)

    def stress_at(level):
        def phase(tile, carry):
            stress_phase(main, level, at_row(tile))
            return carry

        return phase

    def velocity_at(level):
        def phase(tile, carry):
            velocity_phase(main, level, at_row(tile))
            return carry

        return phase

    def put_stress(tile, blocks):
        na, nb, nt = blocks
        r = pl.ds(at_row(tile) - 8, TALL)
        for b in range(nblk):
            l = slice(b * LANES, (b + 1) * LANES)
            out_str[0, r, l] = 0.5 * (na[b] + nb[b])
            out_str[1, r, l] = 0.5 * (na[b] - nb[b])
            out_str[2, r, l] = 0.5 * nt[b]

    def last_stress(tile, carry):
        put_stress(tile, stress_phase(main, ITERS - 1, at_row(tile)))
        return carry

    tall_inner = [None] * nblk
    tall_inner[0] = tall_lane >= 4
    tall_inner[nblk - 1] = tall_lane < LANES - 4

    def last_velocity(tile, carry):
        u, v, nu, nv, inert = velocity_phase(main, ITERS - 1, at_row(tile))
        r = pl.ds(at_row(tile) - 8, TALL)
        for b in range(nblk):
            l = slice(b * LANES, (b + 1) * LANES)
            out_vel[0, r, l] = nu[b]
            out_vel[1, r, l] = nv[b]
        res, kin = square_sums((u, v, nu, nv, inert), tall_inner)
        keep = row_ids(TALL) + tile * TALL
        good = (keep >= 4) & (keep < nrow - 4)
        return carry[0] + jnp.where(good, res, 0.0), carry[1] + jnp.where(good, kin, 0.0)

    zero = jnp.zeros((TALL, LANES), F32)
    wavefront(
        tiles,
        [(6, velocity_at(1)), (4, stress_at(1)), (3, velocity_at(0)), (1, stress_at(0)), (0, prepare)],
        0,
        arrive,
        per // TALL,
        send_rows,
    )

    for copy in row_copies:
        copy.wait()
    no_outside(rows0, gx, ngx)
    for at, to in ((BOT_HALO, nrow), (TOP_HALO - 4, nrow + LANES - 8)):
        ends = [[rows0[f, b, pl.ds(at, 8), :] for f in range(FIELDS)] for b in (0, nblk - 1)]
        for i, x in enumerate(pack(*ends)):
            packed[i, pl.ds(to, 8), :] = x
    for i, names in enumerate((range(SPLIT), range(SPLIT, FIELDS))):
        for blk in range(row_blks + 1):
            flat = packed[i, pl.ds(blk * LANES, LANES), :].T
            for q, f in enumerate(names):
                for at, to in ((16 * q, TOP_OWN), ((16 * q - 8) % LANES, BOT_OWN)):
                    x = flat[at : at + 8, :]
                    cols0[f, blk, pl.ds(to, 8), :] = -x if f == BE else x
    col_copies = exchange(cols0, 1)
    for copy in col_copies:
        copy.start()

    sums = wavefront(
        tiles,
        [(5, last_velocity), (3, last_stress), (2, velocity_at(2)), (0, stress_at(2))],
        (zero, zero),
    )

    def strip_get(first, uv, s):
        def get(field, level):
            if level == 0:
                return first.at[field]
            return uv.at[level - 1, field] if field in (U, V) else s.at[level - 1, field - A]

        return get

    for copy in col_copies:
        copy.wait()
    no_outside(cols0, gy, ngy)
    row_dom = Domain(nblk, strip_get(rows0, rows_uv, rows_s))
    col_dom = Domain(row_blks + 1, strip_get(cols0, cols_uv, cols_s))
    row_ends, col_ends = {}, {}
    for level in range(ITERS):
        for at in (8, 16, 24):
            stress_phase(row_dom, level, at)
            stress_phase(col_dom, level, at)
        for at in (8, 16, 24) if level < ITERS - 1 else (8, 24):
            row_ends[at] = velocity_phase(row_dom, level, at)
            col_ends[at] = velocity_phase(col_dom, level, at)

    def add(sums, more):
        return sums[0] + more[0], sums[1] + more[1]

    sub = row_ids()
    sums = [sum(x[8 * i : 8 * i + 8] for i in range(TALL // 8)) for x in sums]
    inner = [None] * nblk
    inner[0] = lane >= 4
    inner[nblk - 1] = lane < LANES - 4
    for at, good in ((8, sub >= 4), (24, sub < 4)):
        sums = add(sums, square_sums(row_ends[at], [good if m is None else good & m for m in inner]))
        sums = add(sums, square_sums(col_ends[at], [good] * row_blks + [False]))

    half = LANES // 2
    both = [x + pltpu.roll(x, half, 1) for x in sums]
    mine = jnp.where(lane < half, both[0], both[1])
    gather_x[gx, 0:1, :] = jnp.sum(mine, axis=0, keepdims=True)

    def spread(axis, slots, me, count):
        return [
            pltpu.make_async_remote_copy(
                src_ref=slots.at[me, pl.ds(0, 1), :],
                dst_ref=slots.at[me, pl.ds(0, 1), :],
                send_sem=sum_send.at[axis * ngx + d],
                recv_sem=sum_recv.at[axis * ngx + d],
                device_id=peer(axis, d),
                device_id_type=pl.DeviceIdType.MESH,
            )
            for d in range(1, count)
        ]

    x_copies = spread(0, gather_x, gx, ngx)
    for back, at in ((0, TOP_OWN), (8, BOT_OWN)):
        nu, nv = (col_dom.read(f, ITERS, at) for f in (U, V))
        sa, sb, st = (col_dom.read(f, ITERS, at) for f in (A, B, T))
        for blk in range(row_blks):
            values = (
                nv[blk], nu[blk],
                0.5 * (sb[blk] + sa[blk]), 0.5 * (sb[blk] - sa[blk]), 0.5 * st[blk],
            )
            for i, x in enumerate(values):
                turned[blk, pl.ds((16 * i - back) % LANES, 8), :] = x
    for copy in x_copies:
        copy.start()
    for blk in range(row_blks):
        packed[0, pl.ds(blk * LANES, LANES), :] = turned[blk].T
    for at, row, good in ((TOP_OWN, 0, sub < 4), (BOT_OWN, nrow - 8, sub >= 4)):
        nu, nv = (row_dom.read(f, ITERS, at) for f in (U, V))
        sa, sb, st = (row_dom.read(f, ITERS, at) for f in (A, B, T))
        for b in range(nblk):
            r, l = pl.ds(row, 8), slice(b * LANES, (b + 1) * LANES)
            for ref, i, x in (
                (out_vel, 0, nu[b]), (out_vel, 1, nv[b]),
                (out_str, 0, 0.5 * (sa[b] + sb[b])), (out_str, 1, 0.5 * (sa[b] - sb[b])), (out_str, 2, 0.5 * st[b]),
            ):
                ref[i, r, l] = jnp.where(good, x, ref[i, r, l])

    def merge(tile, carry):
        r = pl.ds(pl.multiple_of(tile * 8, 8), 8)
        x = packed[0, r, :]
        places = [((out_vel, i) if i < 2 else (out_str, i - 2)) for i in range(5)]
        first, last = slice(0, LANES), slice(ncol - LANES, ncol)
        new = []
        for i, (ref, at) in enumerate(places):
            edge = pltpu.roll(x, LANES - 16 * i, 1) if i else x
            new.append((ref, at, first, jnp.where(lane < 4, edge, ref[at, r, first])))
            new.append((ref, at, last, jnp.where(lane >= LANES - 4, edge, ref[at, r, last])))
        for ref, at, l, value in new:
            ref[at, r, l] = value
        return carry

    lax.fori_loop(0, nrow // 16, merge, 0, unroll=4)
    for copy in x_copies:
        copy.wait()
    gather_y[gy, 0:1, :] = sum(gather_x[i, 0:1, :] for i in range(ngx))
    y_copies = spread(1, gather_y, gy, ngy)
    for copy in y_copies:
        copy.start()
    lax.fori_loop(nrow // 16, nrow // 8, merge, 0, unroll=4)
    for copy in y_copies:
        copy.wait()
    out_sum[...] = sum(gather_y[i, 0:1, :] for i in range(ngy))


def store_kernel(cells, vel, stress, total, out_vel, out_str, out_res, out_kin, res, kin, sem):
    copies = [pltpu.make_async_copy(vel.at[i], out_vel.at[i], sem.at[i]) for i in range(2)]
    copies += [pltpu.make_async_copy(stress.at[i], out_str.at[i], sem.at[2 + i]) for i in range(3)]
    low = lax.broadcasted_iota(jnp.int32, (1, LANES), 1) < LANES // 2
    both = total[...]
    res[...] = jnp.sum(jnp.where(low, both, 0.0), axis=1, keepdims=True) * (1.0 / cells)
    kin[...] = jnp.sum(jnp.where(low, 0.0, both), axis=1, keepdims=True) * (0.5 * time_step / 4.0 / cells)
    copies += [pltpu.make_async_copy(res, out_res, sem.at[5]), pltpu.make_async_copy(kin, out_kin, sem.at[6])]
    for copy in copies:
        copy.start()
    for copy in copies:
        copy.wait()


def per_device(velocity, stress, strength, ice_mass, wind_stress, current, ice_mask, open_water):
    nrow, ncol = ice_mass.shape
    nblk = ncol // LANES
    row_blks = nrow // LANES
    pad = nrow + 16
    vmem = pltpu.VMEM
    any_spec = pl.BlockSpec(memory_space=pl.ANY)
    vmem_spec = pl.BlockSpec(memory_space=pltpu.VMEM)
    ngx, ngy = lax.axis_size(GX), lax.axis_size(GY)
    new_velocity, new_stress, total = pl.pallas_call(
        main_kernel,
        out_shape=(
            vmem(velocity.shape, F32),
            vmem(stress.shape, F32),
            vmem((1, LANES), F32),
        ),
        in_specs=[any_spec] * 8,
        out_specs=(vmem_spec, vmem_spec, vmem_spec),
        scratch_shapes=[
            vmem((2, nblk, pad, LANES), F32),
            vmem((3, nrow, ncol), F32),
            vmem((nrow, ncol), F32),
            vmem((nrow, ncol), F32),
            vmem((2, nrow, ncol), F32),
            vmem((2, nrow, ncol), F32),
            vmem((nrow, ncol), jnp.int32),
            vmem((nrow, ncol), jnp.int32),
        ]
        + [vmem((2, nblk, pad, LANES), F32)] * ITERS
        + [vmem((3, nblk, pad, LANES), F32)] * (ITERS + 1)
        + [
            vmem((FIELDS - PR, nblk, pad, LANES), F32),
            vmem((2, nrow + LANES, LANES), F32),
            vmem((FIELDS, nblk, STRIP_ROWS, LANES), F32),
            vmem((ITERS, 2, nblk, STRIP_ROWS, LANES), F32),
            vmem((ITERS, 3, nblk, STRIP_ROWS, LANES), F32),
            vmem((FIELDS, row_blks + 1, STRIP_ROWS, LANES), F32),
            vmem((ITERS, 2, row_blks + 1, STRIP_ROWS, LANES), F32),
            vmem((ITERS, 3, row_blks + 1, STRIP_ROWS, LANES), F32),
            vmem((row_blks, LANES, LANES), F32),
            vmem((ngx, 8, LANES), F32),
            vmem((ngy, 8, LANES), F32),
            pltpu.SemaphoreType.DMA((nblk + 7, AHEAD + 1)),
            pltpu.SemaphoreType.DMA((2, 2)),
            pltpu.SemaphoreType.DMA((2, 2)),
            pltpu.SemaphoreType.DMA((ngx + ngy,)),
            pltpu.SemaphoreType.DMA((ngx + ngy,)),
        ],
        compiler_params=pltpu.CompilerParams(
            collective_id=0, has_side_effects=True, vmem_limit_bytes=57 * 1024 * 1024
        ),
        name="subcycles",
    )(velocity, stress, strength, ice_mass, wind_stress, current, ice_mask, open_water)
    new_velocity, new_stress, residual, kinetic = pl.pallas_call(
        functools.partial(store_kernel, nrow * ngx * ncol * ngy),
        out_shape=(
            jax.ShapeDtypeStruct(velocity.shape, F32),
            jax.ShapeDtypeStruct(stress.shape, F32),
            jax.ShapeDtypeStruct((1, 1), F32),
            jax.ShapeDtypeStruct((1, 1), F32),
        ),
        in_specs=[vmem_spec] * 3,
        out_specs=(any_spec,) * 4,
        scratch_shapes=[vmem((1, 1), F32), vmem((1, 1), F32), pltpu.SemaphoreType.DMA((7,))],
        compiler_params=pltpu.CompilerParams(vmem_limit_bytes=1024 * 1024),
        name="store",
    )(new_velocity, new_stress, total)
    return new_velocity, new_stress, residual.reshape(()), kinetic.reshape(())


def solution(mesh):
    split = Mesh(mesh.devices.reshape(4, 2, 2, 4, 2), AXES)
    return jax.shard_map(
        per_device,
        mesh=split,
        in_specs=(
            P(None, GX, GY),
            P(None, GX, GY),
            P(GX, GY),
            P(GX, GY),
            P(None, GX, GY),
            P(None, GX, GY),
            P(GX, GY),
            P(GX, GY),
        ),
        out_specs=(P(None, GX, GY), P(None, GX, GY), P(), P()),
        check_vma=False,
    )
```
